128 devices in a mesh: pp: 2 (over core), dp: 64 (over z, y, x).
Axes of the slice: x: 4, y: 4, z: 4, core: 2. Of those that a mesh axis runs over, the one named last changes fastest.
Arguments:
- x_in: bfloat16 [12, 64, 128, 512], P(None, 'dp')
- seed_grad: bfloat16 [12, 64, 128, 512], P(None, 'dp')
- w_qkv: bfloat16 [4, 512, 1536], P('pp')
- w_out: bfloat16 [4, 512, 512], P('pp')
- w_up: bfloat16 [4, 512, 2048], P('pp')
- w_down: bfloat16 [4, 2048, 512], P('pp')
Outputs:
- output 1: bfloat16 [12, 64, 128, 512], P(None, 'dp')
- output 2: float32 [4, 512, 1536], P('pp', 'dp')
- output 3: float32 [4, 512, 512], P('pp', 'dp')
- output 4: float32 [4, 512, 2048], P('pp', 'dp')
- output 5: float32 [4, 2048, 512], P('pp', 'dp')
All inputs are finite; a program needn't handle non-finite values.
Results may differ from the reference program's by a relative error of at most 0.02.
Values are sent between devices in bfloat16 or wider.
A program may use at most 1 GiB of HBM per device.

```python
import jax
import jax.numpy as jnp
from jax import lax

D_MODEL = 512
HEAD_DIM = 64
LAYERS = 2
MICROBATCHES = 12
BATCH_DEV = 1
SEQ_LEN = 128
STAGES = 2
REPLICAS = 64
NORM_EPS = 1e-6


def setup_inputs(seed: int = 0) -> dict:
    rng_keys = jax.random.split(jax.random.key(seed), 6)
    total_layers = STAGES * LAYERS
    rows_all = REPLICAS * BATCH_DEV
    act_shape = (MICROBATCHES, rows_all, SEQ_LEN, D_MODEL)
    branch = (2.0 * total_layers) ** -0.5
    grad_scale = (MICROBATCHES * rows_all * SEQ_LEN) ** -0.5
    x_in = jax.random.normal(rng_keys[0], act_shape, jnp.float32)
    seed_grad = jax.random.normal(rng_keys[1], act_shape, jnp.float32) * grad_scale
    w_qkv = jax.random.normal(rng_keys[2], (total_layers, D_MODEL, 3 * D_MODEL), jnp.float32) * D_MODEL ** -0.5
    w_out = jax.random.normal(rng_keys[3], (total_layers, D_MODEL, D_MODEL), jnp.float32) * (D_MODEL ** -0.5 * branch)
    w_up = jax.random.normal(rng_keys[4], (total_layers, D_MODEL, 4 * D_MODEL), jnp.float32) * D_MODEL ** -0.5
    w_down = jax.random.normal(rng_keys[5], (total_layers, 4 * D_MODEL, D_MODEL), jnp.float32) * ((4 * D_MODEL) ** -0.5 * branch)
    return {
        "x_in": x_in.astype(jnp.bfloat16),
        "seed_grad": seed_grad.astype(jnp.bfloat16),
        "w_qkv": w_qkv.astype(jnp.bfloat16),
        "w_out": w_out.astype(jnp.bfloat16),
        "w_up": w_up.astype(jnp.bfloat16),
        "w_down": w_down.astype(jnp.bfloat16),
    }


def rms_forward(h_f32):
    return h_f32 * lax.rsqrt(jnp.mean(h_f32 * h_f32, axis=-1, keepdims=True) + NORM_EPS)


def rms_backward(h_f32, grad_f32):
    inv_rms = lax.rsqrt(jnp.mean(h_f32 * h_f32, axis=-1, keepdims=True) + NORM_EPS)
    normed = h_f32 * inv_rms
    return inv_rms * (grad_f32 - normed * jnp.mean(grad_f32 * normed, axis=-1, keepdims=True))


def gelu_tanh(up_f32):
    return jax.nn.gelu(up_f32, approximate=True)


def causal_probs(q_heads, k_heads):
    seq_len = q_heads.shape[1]
    scores = jnp.einsum("bqhe,bkhe->bhqk", q_heads.astype(jnp.float32), k_heads.astype(jnp.float32)) * HEAD_DIM ** -0.5
    allowed = lax.broadcasted_iota(jnp.int32, (seq_len, seq_len), 0) >= lax.broadcasted_iota(jnp.int32, (seq_len, seq_len), 1)
    return jax.nn.softmax(jnp.where(allowed, scores, -1e30), axis=-1)


def layer_forward(h_in, layer_w):
    w_qkv, w_out, w_up, w_down = layer_w
    tokens, model_width = h_in.shape
    head_shape = (tokens // SEQ_LEN, SEQ_LEN, model_width // HEAD_DIM, HEAD_DIM)
    h_f32 = h_in.astype(jnp.float32)
    a_norm = rms_forward(h_f32).astype(jnp.bfloat16)
    qkv_act = jnp.dot(a_norm, w_qkv, preferred_element_type=jnp.float32).astype(jnp.bfloat16)
    q_heads = qkv_act[:, :model_width].reshape(head_shape)
    k_heads = qkv_act[:, model_width:2 * model_width].reshape(head_shape)
    v_heads = qkv_act[:, 2 * model_width:].reshape(head_shape)
    attn_probs = causal_probs(q_heads, k_heads)
    attn_out = jnp.einsum("bhqk,bkhe->bqhe", attn_probs.astype(jnp.bfloat16).astype(jnp.float32), v_heads.astype(jnp.float32)).astype(jnp.bfloat16).reshape(tokens, model_width)
    h_mid = (h_f32 + jnp.dot(attn_out, w_out, preferred_element_type=jnp.float32)).astype(jnp.bfloat16)
    mid_f32 = h_mid.astype(jnp.float32)
    c_norm = rms_forward(mid_f32).astype(jnp.bfloat16)
    up_act = jnp.dot(c_norm, w_up, preferred_element_type=jnp.float32).astype(jnp.bfloat16)
    gelu_act = gelu_tanh(up_act.astype(jnp.float32)).astype(jnp.bfloat16)
    h_out = (mid_f32 + jnp.dot(gelu_act, w_down, preferred_element_type=jnp.float32)).astype(jnp.bfloat16)
    saved_acts = (a_norm, q_heads, k_heads, v_heads, attn_probs, attn_out, h_mid, c_norm, up_act, gelu_act)
    return h_out, saved_acts


def layer_input_grad(d_out, h_in, saved_acts, layer_w):
    w_qkv, w_out, w_up, w_down = layer_w
    a_norm, q_heads, k_heads, v_heads, attn_probs, attn_out, h_mid, c_norm, up_act, gelu_act = saved_acts
    tokens, model_width = d_out.shape
    d_gelu = jnp.dot(d_out, w_down.T, preferred_element_type=jnp.float32)
    gelu_vjp = jax.vjp(gelu_tanh, up_act.astype(jnp.float32))[1]
    d_up = gelu_vjp(d_gelu)[0].astype(jnp.bfloat16)
    d_cnorm = jnp.dot(d_up, w_up.T, preferred_element_type=jnp.float32)
    d_mid = (d_out.astype(jnp.float32) + rms_backward(h_mid.astype(jnp.float32), d_cnorm)).astype(jnp.bfloat16)
    d_attn = jnp.dot(d_mid, w_out.T, preferred_element_type=jnp.float32).astype(jnp.bfloat16).reshape(q_heads.shape)
    d_attn_f32 = d_attn.astype(jnp.float32)
    d_probs = jnp.einsum("bqhe,bkhe->bhqk", d_attn_f32, v_heads.astype(jnp.float32))
    d_vals = jnp.einsum("bhqk,bqhe->bkhe", attn_probs.astype(jnp.bfloat16).astype(jnp.float32), d_attn_f32).astype(jnp.bfloat16)
    d_scores = (attn_probs * (d_probs - jnp.sum(attn_probs * d_probs, axis=-1, keepdims=True)) * HEAD_DIM ** -0.5).astype(jnp.bfloat16)
    d_query = jnp.einsum("bhqk,bkhe->bqhe", d_scores.astype(jnp.float32), k_heads.astype(jnp.float32)).astype(jnp.bfloat16)
    d_key = jnp.einsum("bhqk,bqhe->bkhe", d_scores.astype(jnp.float32), q_heads.astype(jnp.float32)).astype(jnp.bfloat16)
    d_qkv = jnp.concatenate([d_query.reshape(tokens, model_width), d_key.reshape(tokens, model_width), d_vals.reshape(tokens, model_width)], axis=1)
    d_anorm = jnp.dot(d_qkv, w_qkv.T, preferred_element_type=jnp.float32)
    d_in = (d_mid.astype(jnp.float32) + rms_backward(h_in.astype(jnp.float32), d_anorm)).astype(jnp.bfloat16)
    return d_in, (a_norm, d_qkv, attn_out, d_mid, c_norm, d_up, gelu_act, d_out)


def layer_weight_grad(grad_parts):
    a_norm, d_qkv, attn_out, d_mid, c_norm, d_up, gelu_act, d_out = grad_parts
    return (
        jnp.dot(a_norm.T, d_qkv, preferred_element_type=jnp.float32),
        jnp.dot(attn_out.T, d_mid, preferred_element_type=jnp.float32),
        jnp.dot(c_norm.T, d_up, preferred_element_type=jnp.float32),
        jnp.dot(gelu_act.T, d_out, preferred_element_type=jnp.float32),
    )


def reference(x_in, seed_grad, w_qkv, w_out, w_up, w_down):
    num_micro, rows_all, seq_len, model_width = x_in.shape
    tokens = BATCH_DEV * seq_len
    num_chunks = num_micro * rows_all // BATCH_DEV
    x_chunks = x_in.reshape(num_chunks, tokens, model_width)
    g_chunks = seed_grad.reshape(num_chunks, tokens, model_width)
    weights = (w_qkv, w_out, w_up, w_down)

    def forward_layer(h_in, layer_w):
        return layer_forward(h_in, layer_w)[0], h_in

    def backward_layer(d_hid, scan_item):
        h_in, layer_w = scan_item
        saved_acts = layer_forward(h_in, layer_w)[1]
        d_prev, grad_parts = layer_input_grad(d_hid, h_in, saved_acts, layer_w)
        return d_prev, layer_weight_grad(grad_parts)

    def chunk_step(grad_accs, scan_item):
        x_chunk, g_chunk = scan_item
        y_chunk, layer_inputs = lax.scan(forward_layer, x_chunk, weights)
        chunk_grads = lax.scan(backward_layer, g_chunk, (layer_inputs, weights), reverse=True)[1]
        new_accs = tuple(grad_acc + new_grad for grad_acc, new_grad in zip(grad_accs, chunk_grads))
        return new_accs, y_chunk

    zero_accs = tuple(jnp.zeros(weight.shape, jnp.float32) for weight in weights)
    grad_sums, y_chunks = lax.scan(chunk_step, zero_accs, (x_chunks, g_chunks))
    return (y_chunks.reshape(x_in.shape), grad_sums[0], grad_sums[1], grad_sums[2], grad_sums[3])
```

```python
import functools
import math

import jax
import jax.numpy as jnp
from jax import lax
from jax.experimental import pallas as pl
from jax.experimental.pallas import tpu as pltpu
from jax.sharding import PartitionSpec as P

F32 = jnp.float32
BF16 = jnp.bfloat16
MESH = pl.DeviceIdType.MESH

D = 512
HD = 64
LN = 128
TILE = (8, LN)
NU = 6
SEQ = LN
NSEQ = 6
ROWS = NSEQ * SEQ
LAYERS = 4
EPS = 1e-6
GELU_C1 = math.sqrt(2.0 / math.pi)
GELU_C2 = GELU_C1 * 0.044715
EXP2_SCALE = HD ** -0.5 * math.log2(math.e)
W_SHAPES = ((D, 3 * D), (D, D), (D, 4 * D), (4 * D, D))
LAST = (((1,), (1,)), ((), ()))
FIRST = (((0,), (0,)), ((), ()))


def dot(a, b):
    return jnp.dot(a, b, preferred_element_type=F32)


def dot_last(a, b):
    return lax.dot_general(a, b, LAST, preferred_element_type=F32)


def dot_first(a, b):
    return lax.dot_general(a, b, FIRST, preferred_element_type=F32)


def inv_rms(h):
    return lax.rsqrt(jnp.mean(h * h, axis=-1, keepdims=True) + EPS)


def rms_bwd(h, g):
    ir = inv_rms(h)
    n = h * ir
    return ir * (g - n * jnp.mean(g * n, axis=-1, keepdims=True))


def gelu(u):
    t = jnp.tanh(u * (GELU_C1 + GELU_C2 * (u * u)))
    hu = 0.5 * u
    return hu + hu * t


def gelu_and_slope(u):
    a = GELU_C2 * (u * u)
    t = jnp.tanh(u * (a + GELU_C1))
    hu = 0.5 * u
    ht = hu * t
    return hu + ht, (0.5 * t + 0.5) + (hu - ht * t) * (3.0 * a + GELU_C1)


def block_diag(x):
    first = lax.broadcasted_iota(jnp.int32, (SEQ, 2 * HD), 1) < HD
    zero = jnp.zeros_like(x)
    return jnp.concatenate([jnp.where(first, x, zero), jnp.where(first, zero, x)], axis=0)


def units_of(step, n_seqs):
    return [(pl.ds(pl.multiple_of((step * n_seqs + n) * SEQ, SEQ), SEQ), pair) for n in range(n_seqs) for pair in range(4)]


def attention_fwd(step, n_seqs, qkv, p_out, o_out):
    key = lax.broadcasted_iota(jnp.int32, (SEQ, SEQ), 0)
    query = lax.broadcasted_iota(jnp.int32, (SEQ, SEQ), 1)
    allowed = key <= query
    units = units_of(step, n_seqs)

    def scores(rows, pair):
        c = pair * LN
        return dot_last(qkv[rows, D + c:D + c + LN], block_diag(qkv[rows, c:c + LN]))

    ahead = 2
    pending = [scores(*u) for u in units[:ahead]]
    for i, (rows, pair) in enumerate(units):
        if i + ahead < len(units):
            pending.append(scores(*units[i + ahead]))
        s = pending[i]
        c = pair * LN
        probs = []
        for head in range(2):
            sh = jnp.where(allowed, s[:, head * LN:head * LN + LN], -1e30)
            e = jnp.exp2((sh - jnp.max(sh, axis=0, keepdims=True)) * EXP2_SCALE)
            p = e * (1.0 / jnp.sum(e, axis=0, keepdims=True))
            p_out[rows, 2 * c + head * LN:2 * c + head * LN + LN] = p
            probs.append(p.astype(BF16))
        v = qkv[rows, 2 * D + c:2 * D + c + LN]
        o_out[rows, c:c + LN] = dot_first(jnp.concatenate(probs, axis=0), block_diag(v)).astype(BF16)


def attention_bwd(step, n_seqs, qkv, p_in, do):
    units = units_of(step, n_seqs)

    def first(rows, pair):
        c = pair * LN
        d = block_diag(do[rows, c:c + LN])
        return d, dot_last(qkv[rows, 2 * D + c:2 * D + c + LN], d)

    ahead = 2
    pending = [first(*u) for u in units[:ahead]]
    for i, (rows, pair) in enumerate(units):
        if i + ahead < len(units):
            pending.append(first(*units[i + ahead]))
        d, dp = pending[i]
        c = pair * LN
        q = qkv[rows, c:c + LN]
        k = qkv[rows, D + c:D + c + LN]
        p = p_in[rows, 2 * c:2 * c + 256]
        dv = dot(p.astype(BF16), d).astype(BF16)
        pd = p * dp
        ds = ((pd - p * jnp.sum(pd, axis=0, keepdims=True)) * HD ** -0.5).astype(BF16)
        dk = dot(ds, block_diag(q)).astype(BF16)
        dq = dot_first(jnp.concatenate([ds[:, :LN], ds[:, LN:]], axis=0), block_diag(k)).astype(BF16)
        qkv[rows, c:c + LN] = dq
        qkv[rows, D + c:D + c + LN] = dk
        qkv[rows, 2 * D + c:2 * D + c + LN] = dv


AXES = (("x", "y", "z"), ("y", "z", "x"), ("z", "x", "y"))
NAT = ("z", "y", "x")
STRIDE = {"x": 1, "y": 4, "z": 16}
UNITS = [(colour, way) for colour in range(3) for way in (1, -1)]


class Place:
    def __init__(self):
        self.core = lax.axis_index("pp")
        self.dp = lax.axis_index("dp")
        self.at = {"x": lax.rem(self.dp, 4), "y": lax.rem(self.dp // 4, 4), "z": self.dp // 16}

    def neighbour(self, axis, way):
        c = self.at[axis]
        return (self.core, self.dp + (lax.rem(c + way + 4, 4) - c) * STRIDE[axis])

    def partner(self):
        return (1 - self.core, self.dp)

    def block(self, axis, way, step):
        return lax.rem(self.at[axis] - way * (1 + step) + 8, 4)


def greet(peers):
    barrier = pltpu.get_barrier_semaphore()
    for p in peers:
        pl.semaphore_signal(barrier, inc=1, device_id=p, device_id_type=MESH)
    pl.semaphore_wait(barrier, len(peers))


FWD_SEQS = 3


def forward_kernel(x, wq, wo, wu, wd, y, rq, ro, ru, rd, hs, qs, ps, os, ms, us,
                   h, qkv, p, o, m, u, vq, vo, vu, vd, wsem, psem, qsem, osem, ysem, hsem):
    place = Place()
    core = place.core
    mine = (wq, wo, wu, wd)
    theirs = (rq, ro, ru, rd)
    held = (vq, vo, vu, vd)

    def push(k, j):
        return pltpu.make_async_remote_copy(mine[k].at[j], theirs[k].at[j], psem.at[k, j], qsem.at[k, j],
                                            device_id=place.partner(), device_id_type=MESH)

    def fetch(k, l):
        local = lax.rem(l, 2)

        @pl.when(l // 2 == core)
        def _():
            pltpu.make_async_copy(mine[k].at[local], held[k].at[local], wsem.at[k, local]).start()

        @pl.when(l // 2 != core)
        def _():
            push(k, local).wait_recv()
            pltpu.make_async_copy(theirs[k].at[local], held[k].at[local], wsem.at[k, local]).start()

    def weight(k, l):
        local = lax.rem(l, 2)
        pltpu.make_async_copy(mine[k].at[0], held[k].at[local], wsem.at[k, local]).wait()
        return held[k].at[local]

    saved = ((h, hs), (qkv, qs), (p, ps), (o, os), (m, ms), (u, us))

    def save(i, l):
        src, dst = saved[i]
        return pltpu.make_async_copy(src.at[lax.rem(l, 2)] if i == 0 else src, dst.at[l], osem.at[i])

    first = pltpu.make_async_copy(x.at[pl.ds(core * ROWS, ROWS)], h.at[0], hsem)
    first.start()
    greet([place.partner()])
    for j in range(2):
        for k in range(4):
            push(k, j).start()
    fetch(0, 0)
    fetch(1, 0)
    first.wait()

    def layer(l, _):
        now, later = lax.rem(l, 2), lax.rem(l + 1, 2)

        def again(i):
            @pl.when(l > 0)
            def _():
                save(i, l - 1).wait()

        w = weight(0, l)
        hf = h[now].astype(F32)
        a = (hf * inv_rms(hf)).astype(BF16)
        again(0)
        save(0, l).start()
        again(1)
        qkv[...] = dot(a, w[...]).astype(BF16)
        save(1, l).start()
        again(2)
        again(3)

        def attend(i, _):
            attention_fwd(i, FWD_SEQS, qkv, p, o)
            return 0

        lax.fori_loop(0, NSEQ // FWD_SEQS, attend, 0)
        save(2, l).start()
        save(3, l).start()

        @pl.when(l == 0)
        def _():
            fetch(2, 0)
            fetch(3, 0)

        @pl.when(l < LAYERS - 1)
        def _():
            fetch(0, l + 1)
            fetch(1, l + 1)

        w = weight(1, l)
        again(4)
        mb = (h[now].astype(F32) + dot(o[...], w[...])).astype(BF16)
        m[...] = mb
        save(4, l).start()
        wup, wdn = weight(2, l), weight(3, l)
        again(5)
        mf = m[...].astype(F32)
        c = (mf * inv_rms(mf)).astype(BF16)
        acc = mf
        for j in range(2):
            cols = slice(j * 2 * D, (j + 1) * 2 * D)
            ub = dot(c, wup[:, cols]).astype(BF16)
            u[:, cols] = ub
            acc = acc + dot(gelu(ub.astype(F32)).astype(BF16), wdn[cols, :])
        h[later] = acc.astype(BF16)
        save(5, l).start()

        @pl.when(l < LAYERS - 1)
        def _():
            fetch(2, l + 1)
            fetch(3, l + 1)
        return 0

    lax.fori_loop(0, LAYERS, layer, 0)
    rows = pl.ds(core * ROWS, ROWS)
    out = pltpu.make_async_copy(h.at[0], y.at[rows], ysem.at[0])
    cross = pltpu.make_async_remote_copy(h.at[0], y.at[rows], ysem.at[1], ysem.at[2],
                                         device_id=place.partner(), device_id_type=MESH)
    out.start()
    cross.start()
    for i in range(NU):
        save(i, LAYERS - 1).wait()
    for j in range(2):
        for k in range(4):
            push(k, j).wait_send()
    out.wait()
    cross.wait_send()
    cross.wait_recv()


def forward(x, weights):
    act = lambda cols, dt=BF16: jax.ShapeDtypeStruct((LAYERS, ROWS, cols), dt)
    other = [jax.ShapeDtypeStruct((2,) + s, BF16) for s in W_SHAPES]
    anywhere = pl.BlockSpec(memory_space=pl.ANY)
    return pl.pallas_call(
        forward_kernel,
        name="forward",
        out_shape=[jax.ShapeDtypeStruct((2 * ROWS, D), BF16)] + other
        + [act(D), act(3 * D), act(2 * D, F32), act(D), act(D), act(4 * D)],
        in_specs=[anywhere] * 5,
        out_specs=[anywhere] * 11,
        scratch_shapes=[
            pltpu.VMEM((2, ROWS, D), BF16), pltpu.VMEM((ROWS, 3 * D), BF16), pltpu.VMEM((ROWS, 2 * D), F32),
            pltpu.VMEM((ROWS, D), BF16), pltpu.VMEM((ROWS, D), BF16), pltpu.VMEM((ROWS, 4 * D), BF16),
        ] + [pltpu.VMEM((2,) + s, BF16) for s in W_SHAPES] + [
            pltpu.SemaphoreType.DMA((4, 2)), pltpu.SemaphoreType.DMA((4, 2)), pltpu.SemaphoreType.DMA((4, 2)),
            pltpu.SemaphoreType.DMA((6,)), pltpu.SemaphoreType.DMA((3,)), pltpu.SemaphoreType.DMA,
        ],
        compiler_params=pltpu.CompilerParams(collective_id=1, has_side_effects=True, vmem_limit_bytes=60 * 2 ** 20),
    )(x, *weights)


CHUNKS = 16
STREAMS = 4
POS = {1: 0, 0: 1, 3: 2, 2: 3}
J0 = {1: 0, 0: 1, 3: 1, 2: 2}


def ring_scratch():
    return [
        pltpu.VMEM((STREAMS, 6, 4, 4, *TILE), F32), pltpu.VMEM((STREAMS, 2, 6, 4, 4, *TILE), F32),
        pltpu.VMEM((STREAMS, 6, 4, 4, *TILE), F32),
        pltpu.VMEM((STREAMS, 6, 4, *TILE), F32), pltpu.VMEM((STREAMS, 2, 6, 4, *TILE), F32),
        pltpu.VMEM((STREAMS, 6, 4, *TILE), F32),
        pltpu.VMEM((STREAMS, 6, *TILE), F32), pltpu.VMEM((STREAMS, 2, 6, *TILE), F32),
        pltpu.SemaphoreType.DMA((STREAMS, 3, 2, 6)), pltpu.SemaphoreType.DMA((STREAMS, 3, 2, 6)),
    ]


def pick_block(ref, axis, b):
    return {"z": lambda: ref[b], "y": lambda: ref[:, b], "x": lambda: ref[:, :, b]}[axis]()


class Rings:
    def __init__(self, place, scratch, own, ready, done):
        self.p, self.own, self.ready, self.done = place, own, ready, done
        (self.s1, self.r1, self.t1, self.s2, self.r2, self.t2, self.s3, self.r3, self.ss, self.rs) = scratch

    def copy(self, e, phase, par, u):
        colour, way = UNITS[u]
        src = (self.s1, self.s2, self.s3)[phase].at[e, u]
        dst = (self.r1, self.r2, self.r3)[phase].at[e, par, u]
        return pltpu.make_async_remote_copy(src, dst, self.ss.at[e, phase, par, u], self.rs.at[e, phase, par, u],
                                            device_id=self.p.neighbour(AXES[colour][phase], way), device_id_type=MESH)

    def wait(self, e, phase, par):
        for u in range(NU):
            c = self.copy(e, phase, par, u)
            c.wait_send()
            c.wait_recv()

    def send(self, e, phase, par):
        for u in range(NU):
            self.copy(e, phase, par, u).start()

    def block(self, u, phase, step):
        colour, way = UNITS[u]
        return self.p.block(AXES[colour][phase], way, step)

    def own_block(self, ref, u, step):
        return pick_block(ref.at[u], AXES[UNITS[u][0]][0], self.block(u, 0, step))

    def second(self, e, u, step):
        order = AXES[UNITS[u][0]]
        b = self.block(u, 1, step)
        rest = [a for a in NAT if a != order[0]]
        return self.t1[e, u, :, b] if rest.index(order[1]) == 1 else self.t1[e, u, b]

    def third(self, e, u, step):
        return self.t2[e, u, self.block(u, 2, step)]

    def slot(self, n, iteration):
        e, j = n % STREAMS, n // STREAMS
        step = (j - J0[e]) % 3
        k = iteration + (j - J0[e]) // 3
        tick = lax.rem(3 * iteration + j, 2)
        par, old = tick, 1 - tick
        chunk = lambda i: STREAMS * (k - i) + POS[e] - 1
        live = lambda i: (chunk(i) >= 0) & (chunk(i) < CHUNKS)
        if step == 0:
            @pl.when(live(3))
            def _():
                self.wait(e, 2, old)
                for u in range(NU):
                    self.done[chunk(3), u] = self.r3[e, old, u] + self.third(e, u, 3)

            @pl.when(live(2))
            def _():
                self.wait(e, 1, old)
                for u in range(NU):
                    self.t2[e, u] = self.r2[e, old, u] + self.second(e, u, 3)
                    self.s3[e, u] = self.third(e, u, 0)

            @pl.when(live(1))
            def _():
                self.wait(e, 0, old)
                own = self.own(chunk(1))
                for u in range(NU):
                    self.t1[e, u] = self.r1[e, old, u] + self.own_block(own, u, 3)
                    self.s2[e, u] = self.second(e, u, 0)

            @pl.when(live(0))
            def _():
                self.ready(chunk(0))
                own = self.own(chunk(0))
                for u in range(NU):
                    self.s1[e, u] = self.own_block(own, u, 0)
        else:
            @pl.when(live(2))
            def _():
                self.wait(e, 2, old)
                for u in range(NU):
                    self.s3[e, u] = self.r3[e, old, u] + self.third(e, u, step)

            @pl.when(live(1))
            def _():
                self.wait(e, 1, old)
                for u in range(NU):
                    self.s2[e, u] = self.r2[e, old, u] + self.second(e, u, step)

            @pl.when(live(0))
            def _():
                self.wait(e, 0, old)
                own = self.own(chunk(0))
                for u in range(NU):
                    self.s1[e, u] = self.r1[e, old, u] + self.own_block(own, u, step)
        for phase in range(3):
            @pl.when(live(phase))
            def _():
                self.send(e, phase, par)


def tiles_of_layer():
    down = [(3, g, j) for j in range(4) for g in range(4)]
    up = [(2, 0, j) for j in range(16)]
    out = [(1, 0, j) for j in range(4)]
    qkv = [(0, 0, j) for j in range(12)]
    return down + up + out + qkv


TILES = tiles_of_layer()
PLACE_OF = {t: (i // 12, i % 12 // 6, i % 6) for i, t in enumerate(TILES)}


BWD_SEQS = 2
OWN_SLOTS = 8
DRAIN = 4


def backward_kernel(seed, wq, wo, wu, wd, rq, ro, ru, rd, hs, qs, ps, os, ms, us,
                    gq, go, gu, gd,
                    grads, recv, done, done_rx, h, qkv, p, o, m, u, e, g, g1, do, vq, vo, vu, vd,
                    wsem, asem, gsem, dsend, drecv, fsem, credit, *ring):
    place = Place()
    core = place.core
    mine = (wq, wo, wu, wd)
    theirs = (rq, ro, ru, rd)
    held = (vq, vo, vu, vd)
    acts = ((h, hs), (qkv, qs), (p, ps), (o, os), (m, ms), (u, us))
    H, QKV, PROB, O, M, U = range(6)

    def fetch_w(k, l):
        for c in range(2):
            src = (mine if c == 0 else theirs)[k]

            @pl.when((l // 2 == core) if c == 0 else (l // 2 != core))
            def _():
                pltpu.make_async_copy(src.at[lax.rem(l, 2)], held[k], wsem.at[k]).start()

    def wait_w(k):
        pltpu.make_async_copy(mine[k].at[0], held[k], wsem.at[k]).wait()

    def act(i, l):
        dst, src = acts[i]
        return pltpu.make_async_copy(src.at[l], dst, asem.at[i])

    def own_slot(chunk):
        return lax.rem(chunk, OWN_SLOTS)

    def cross(chunk):
        q = lax.rem(chunk, 4)
        return pltpu.make_async_remote_copy(grads.at[OWN_SLOTS + q], recv.at[q], dsend.at[q], drecv.at[q],
                                            device_id=place.partner(), device_id_type=MESH)

    def ready(chunk):
        q = lax.rem(chunk, 4)
        cross(chunk).wait_recv()
        for unit in range(NU):
            grads[own_slot(chunk), unit] = grads[own_slot(chunk), unit] + recv[q, unit]

        @pl.when(chunk + 4 < CHUNKS)
        def _():
            pl.semaphore_signal(credit.at[q], inc=1, device_id=place.partner(), device_id_type=MESH)

    rings = Rings(place, ring, lambda chunk: grads.at[own_slot(chunk)], ready, done)

    seed_in = pltpu.make_async_copy(seed.at[pl.ds(core * ROWS, ROWS)], g, gsem)
    seed_in.start()
    for k in (3, 2):
        fetch_w(k, LAYERS - 1)
    for i in (U, M, O, PROB, QKV, H):
        act(i, LAYERS - 1).start()
    for k in (1, 0):
        fetch_w(k, LAYERS - 1)
    greet([place.partner()] + [place.neighbour(a, way) for a in NAT for way in (1, -1)])
    seed_in.wait()

    def iteration(it, _):
        l = LAYERS - 1 - it
        busy = it < LAYERS
        more = it < LAYERS - 1
        base = 4 * it

        def free(q):
            @pl.when(it > 0)
            def _():
                cross(base - 4 + q).wait_send()

        def put(array, row_group, col, value):
            q, half, unit = PLACE_OF[array, row_group, col]
            index = jnp.where(core == half, own_slot(base + q), OWN_SLOTS + q)
            grads[index, unit] = value.reshape(4, 4, 4, *TILE)

        def ship(q):
            @pl.when(it > 0)
            def _():
                pl.semaphore_wait(credit.at[q], 1)
            cross(base + q).start()

        def gelu_part(j):
            cols = slice(j * D, (j + 1) * D)
            de = dot_last(g[...], vd[cols, :])
            ej, slope = gelu_and_slope(u[:, cols].astype(F32))
            e[:, cols] = ej.astype(BF16)
            u[:, cols] = (slope * de).astype(BF16)

        def piece(n):
            if n == 0:
                wait_w(3)
                act(U, l).wait()
                gelu_part(0)
                gelu_part(1)
            elif n == 1:
                gelu_part(2)
                gelu_part(3)

                @pl.when(more)
                def _():
                    fetch_w(3, l - 1)
            elif n == 2:
                free(0)
                free(1)
                for half in range(2):
                    w = dot_first(e[...], g[:, half * 256:half * 256 + 256]).reshape(64, 4, 8, 256)
                    for j in range(2):
                        for rg in range(4):
                            put(3, rg, 2 * half + j, w[:, rg, :, j * LN:j * LN + LN])
                ship(0)
            elif n == 3:
                wait_w(2)
                act(M, l).wait()
                dc = dot_last(u[...], vu[...])
                g1[...] = (g[...].astype(F32) + rms_bwd(m[...].astype(F32), dc)).astype(BF16)

                @pl.when(more)
                def _():
                    fetch_w(2, l - 1)
            elif n == 4:
                free(2)
                mf = m[...].astype(F32)
                c = (mf * inv_rms(mf)).astype(BF16)
                for part in range(4):
                    w = dot_first(c, u[:, part * D:part * D + D]).reshape(64, 8, D)
                    for j in range(4):
                        put(2, 0, 4 * part + j, w[:, :, j * LN:j * LN + LN])
                ship(1)

                @pl.when(more)
                def _():
                    act(U, l - 1).start()
                    act(M, l - 1).start()
            elif n == 5:
                wait_w(1)
                act(O, l).wait()
                do[...] = dot_last(g1[...], vo[...]).astype(BF16)
                w = dot_first(o[...], g1[...]).reshape(64, 8, D)
                for j in range(4):
                    put(1, 0, j, w[:, :, j * LN:j * LN + LN])
                ship(2)

                @pl.when(more)
                def _():
                    fetch_w(1, l - 1)
                    act(O, l - 1).start()
            elif n in (6, 7, 8):
                if n == 6:
                    act(PROB, l).wait()
                    act(QKV, l).wait()
                attention_bwd(n - 6, BWD_SEQS, qkv, p, do)
                if n == 8:
                    @pl.when(more)
                    def _():
                        act(PROB, l - 1).start()
            elif n == 9:
                wait_w(0)
                act(H, l).wait()
                da = dot_last(qkv[...], vq[...])
                g[...] = (g1[...].astype(F32) + rms_bwd(h[...].astype(F32), da)).astype(BF16)

                @pl.when(more)
                def _():
                    fetch_w(0, l - 1)
            elif n == 10:
                free(3)
                hf = h[...].astype(F32)
                a = (hf * inv_rms(hf)).astype(BF16)
                for part in range(3):
                    w = dot_first(a, qkv[:, part * D:part * D + D]).reshape(64, 8, D)
                    for j in range(4):
                        put(0, 0, 4 * part + j, w[:, :, j * LN:j * LN + LN])
                ship(3)

                @pl.when(more)
                def _():
                    act(H, l - 1).start()
                    act(QKV, l - 1).start()

        for n in range(12):
            if n < 11:
                @pl.when(busy)
                def _():
                    piece(n)
            rings.slot(n, it)
        return 0

    lax.fori_loop(0, LAYERS + DRAIN, iteration, 0)
    for q in range(4):
        cross(CHUNKS - 4 + q).wait_send()

    kept = 8 * (1 - core)
    last = pltpu.make_async_remote_copy(done.at[pl.ds(8 * core, 8)], done_rx, fsem.at[0], fsem.at[1],
                                        device_id=place.partner(), device_id_type=MESH)
    last.start()
    last.wait_send()
    last.wait_recv()
    outs = (gq, go, gu, gd)
    for layer in range(2):
        for tile in TILES:
            array, rg, col = tile
            q, half, unit = PLACE_OF[tile]
            i = 4 * (1 - layer) + q
            value = jnp.where(core == half, done[kept + i, unit], done_rx[i, unit])
            outs[array][layer, rg * 8:rg * 8 + 8, col * LN:col * LN + LN] = value


def backward(seed, weights, saved):
    anywhere = pl.BlockSpec(memory_space=pl.ANY)
    vmem = pl.BlockSpec(memory_space=pltpu.VMEM)
    act = lambda cols, dt=BF16: pltpu.VMEM((ROWS, cols), dt)
    return pl.pallas_call(
        backward_kernel,
        name="backward",
        out_shape=[jax.ShapeDtypeStruct(s, F32) for s in ((2, 8, 3 * D), (2, 8, D), (2, 8, 4 * D), (2, 32, D))],
        in_specs=[anywhere] * 15,
        out_specs=[vmem] * 4,
        scratch_shapes=[
            pltpu.VMEM((OWN_SLOTS + 4, 6, 4, 4, 4, *TILE), F32),
            pltpu.VMEM((4, 6, 4, 4, 4, *TILE), F32),
            pltpu.VMEM((CHUNKS, 6, *TILE), F32), pltpu.VMEM((8, 6, *TILE), F32),
            act(D), act(3 * D), act(2 * D, F32), act(D), act(D), act(4 * D), act(4 * D), act(D), act(D), act(D),
        ] + [pltpu.VMEM(s, BF16) for s in W_SHAPES] + [
            pltpu.SemaphoreType.DMA((4,)), pltpu.SemaphoreType.DMA((6,)), pltpu.SemaphoreType.DMA,
            pltpu.SemaphoreType.DMA((4,)), pltpu.SemaphoreType.DMA((4,)), pltpu.SemaphoreType.DMA((2,)),
            pltpu.SemaphoreType.REGULAR((4,)),
        ] + ring_scratch(),
        compiler_params=pltpu.CompilerParams(collective_id=2, has_side_effects=True, vmem_limit_bytes=67043328),
    )(seed, *weights, *saved)


def solution(mesh):
    def step(x_in, seed_grad, w_qkv, w_out, w_up, w_down):
        shape = x_in.shape
        weights = (w_qkv, w_out, w_up, w_down)
        y, *saved = forward(x_in.reshape(2 * ROWS, D), weights)
        gq, go, gu, gd = backward(seed_grad.reshape(2 * ROWS, D), weights, saved)
        return y.reshape(shape), gq, go, gu, gd

    act, weight, grad = P(None, "dp"), P("pp"), P("pp", "dp")
    return jax.shard_map(
        step,
        mesh=mesh,
        in_specs=(act, act, weight, weight, weight, weight),
        out_specs=(act, grad, grad, grad, grad),
        check_vma=False,
    )
```

```python
import functools
import math

import jax
import jax.numpy as jnp
from jax import lax
from jax.experimental import pallas as pl
from jax.experimental.pallas import tpu as pltpu
from jax.sharding import PartitionSpec as P

F32 = jnp.float32
BF16 = jnp.bfloat16
MESH = pl.DeviceIdType.MESH

D = 512
HD = 64
LN = 128
TILE = (8, LN)
NU = 6
SEQ = LN
NSEQ = 6
ROWS = NSEQ * SEQ
LAYERS = 4
EPS = 1e-6
GELU_C1 = math.sqrt(2.0 / math.pi)
GELU_C2 = GELU_C1 * 0.044715
EXP2_SCALE = HD ** -0.5 * math.log2(math.e)
W_SHAPES = ((D, 3 * D), (D, D), (D, 4 * D), (4 * D, D))
LAST = (((1,), (1,)), ((), ()))
FIRST = (((0,), (0,)), ((), ()))


def dot(a, b):
    return jnp.dot(a, b, preferred_element_type=F32)


def dot_last(a, b):
    return lax.dot_general(a, b, LAST, preferred_element_type=F32)


def dot_first(a, b):
    return lax.dot_general(a, b, FIRST, preferred_element_type=F32)


def inv_rms(h):
    return lax.rsqrt(jnp.mean(h * h, axis=-1, keepdims=True) + EPS)


def rms_bwd(h, g):
    ir = inv_rms(h)
    n = h * ir
    return ir * (g - n * jnp.mean(g * n, axis=-1, keepdims=True))


def gelu(u):
    t = jnp.tanh(u * (GELU_C1 + GELU_C2 * (u * u)))
    return u * (0.5 * t + 0.5)


def gelu_and_slope(u):
    a = GELU_C2 * (u * u)
    t = jnp.tanh(u * (a + GELU_C1))
    half = 0.5 * t + 0.5
    e = u * half
    return e, half + e * (1.0 - t) * (3.0 * a + GELU_C1)


def block_diag(x):
    first = lax.broadcasted_iota(jnp.int32, (SEQ, 2 * HD), 1) < HD
    zero = jnp.zeros_like(x)
    return jnp.concatenate([jnp.where(first, x, zero), jnp.where(first, zero, x)], axis=0)


def units_of(step, n_seqs):
    return [(pl.ds(pl.multiple_of((step * n_seqs + n) * SEQ, SEQ), SEQ), pair) for n in range(n_seqs) for pair in range(4)]


def attention_fwd(step, n_seqs, qkv, p_out, o_out):
    key = lax.broadcasted_iota(jnp.int32, (SEQ, SEQ), 0)
    query = lax.broadcasted_iota(jnp.int32, (SEQ, SEQ), 1)
    allowed = key <= query
    units = units_of(step, n_seqs)

    def scores(rows, pair):
        c = pair * LN
        return dot_last(qkv[rows, D + c:D + c + LN], block_diag(qkv[rows, c:c + LN]))

    ahead = 2
    pending = [scores(*u) for u in units[:ahead]]
    for i, (rows, pair) in enumerate(units):
        if i + ahead < len(units):
            pending.append(scores(*units[i + ahead]))
        s = pending[i]
        c = pair * LN
        probs = []
        for head in range(2):
            sh = jnp.where(allowed, s[:, head * LN:head * LN + LN], -1e30)
            e = jnp.exp2((sh - jnp.max(sh, axis=0, keepdims=True)) * EXP2_SCALE)
            p = e * (1.0 / jnp.sum(e, axis=0, keepdims=True))
            p_out[rows, 2 * c + head * LN:2 * c + head * LN + LN] = p
            probs.append(p.astype(BF16))
        v = qkv[rows, 2 * D + c:2 * D + c + LN]
        o_out[rows, c:c + LN] = dot_first(jnp.concatenate(probs, axis=0), block_diag(v)).astype(BF16)


def attention_bwd(step, n_seqs, qkv, p_in, do):
    units = units_of(step, n_seqs)

    def first(rows, pair):
        c = pair * LN
        d = block_diag(do[rows, c:c + LN])
        return d, dot_last(qkv[rows, 2 * D + c:2 * D + c + LN], d)

    ahead = 2
    pending = [first(*u) for u in units[:ahead]]
    for i, (rows, pair) in enumerate(units):
        if i + ahead < len(units):
            pending.append(first(*units[i + ahead]))
        d, dp = pending[i]
        c = pair * LN
        q = qkv[rows, c:c + LN]
        k = qkv[rows, D + c:D + c + LN]
        p = p_in[rows, 2 * c:2 * c + 256]
        dv = dot(p.astype(BF16), d).astype(BF16)
        pd = p * dp
        ds = ((pd - p * jnp.sum(pd, axis=0, keepdims=True)) * HD ** -0.5).astype(BF16)
        dk = dot(ds, block_diag(q)).astype(BF16)
        dq = dot_first(jnp.concatenate([ds[:, :LN], ds[:, LN:]], axis=0), block_diag(k)).astype(BF16)
        qkv[rows, c:c + LN] = dq
        qkv[rows, D + c:D + c + LN] = dk
        qkv[rows, 2 * D + c:2 * D + c + LN] = dv


AXES = (("x", "y", "z"), ("y", "z", "x"), ("z", "x", "y"))
NAT = ("z", "y", "x")
STRIDE = {"x": 1, "y": 4, "z": 16}
UNITS = [(colour, way) for colour in range(3) for way in (1, -1)]


class Place:
    def __init__(self):
        self.core = lax.axis_index("pp")
        self.dp = lax.axis_index("dp")
        self.at = {"x": lax.rem(self.dp, 4), "y": lax.rem(self.dp // 4, 4), "z": self.dp // 16}

    def neighbour(self, axis, way):
        c = self.at[axis]
        return (self.core, self.dp + (lax.rem(c + way + 4, 4) - c) * STRIDE[axis])

    def partner(self):
        return (1 - self.core, self.dp)

    def block(self, axis, way, step):
        return lax.rem(self.at[axis] - way * (1 + step) + 8, 4)


def greet(peers):
    barrier = pltpu.get_barrier_semaphore()
    for p in peers:
        pl.semaphore_signal(barrier, inc=1, device_id=p, device_id_type=MESH)
    pl.semaphore_wait(barrier, len(peers))


CHUNKS = 16
STREAMS = 4
POS = {0: 0, 3: 1, 2: 2, 1: 3}
J0 = {0: 0, 3: 0, 2: 1, 1: 2}


HOP = (16, 4, 1)
FROM = (0, 16, 20)
LINK = 21


def ring_scratch():
    return [
        pltpu.VMEM((STREAMS, NU, LINK) + TILE, F32), pltpu.VMEM((STREAMS, 2, NU, LINK) + TILE, F32),
        pltpu.VMEM((STREAMS, NU, 4, 4) + TILE, F32), pltpu.VMEM((STREAMS, NU, 4) + TILE, F32),
        pltpu.SemaphoreType.DMA((STREAMS,)), pltpu.SemaphoreType.DMA((STREAMS, 2)),
    ]


def pick_block(ref, axis, b):
    return {"z": lambda: ref[b], "y": lambda: ref[:, b], "x": lambda: ref[:, :, b]}[axis]()


class Rings:
    def __init__(self, place, scratch, own, ready, done):
        self.p, self.own, self.ready, self.done = place, own, ready, done
        self.sent, self.got, self.t1, self.t2, self.ss, self.rs = scratch
        self.sent[:, :, FROM[1]:] = jnp.zeros((STREAMS, NU, LINK - FROM[1]) + TILE, F32)

    def links(self, e, par, link, lo):
        tiles = pl.ds(lo, LINK - lo)
        axis, way = UNITS[0 if link is None else link]
        at = slice(None) if link is None else link
        return pltpu.make_async_remote_copy(self.sent.at[e, at, tiles], self.got.at[e, par, at, tiles], self.ss.at[e], self.rs.at[e, par],
                                            device_id=self.p.neighbour("xyz"[axis], way), device_id_type=MESH)

    def wait(self, e, par, lo):
        c = self.links(e, par, None, lo)
        c.wait_send()
        c.wait_recv()

    def send(self, e, par, lo):
        for link in range(NU):
            self.links(e, par, link, lo).start()

    def link(self, u, phase):
        return (u + 2 * phase) % NU

    def came(self, e, par, u, phase):
        lo = FROM[phase]
        v = self.got[e, par, self.link(u, phase), lo:lo + HOP[phase]]
        return v.reshape(((4, 4), (4,), ())[phase] + TILE)

    def go(self, e, u, phase, value):
        lo = FROM[phase]
        self.sent[e, self.link(u, phase), lo:lo + HOP[phase]] = value.reshape((HOP[phase],) + TILE)

    def block(self, u, phase, step):
        colour, way = UNITS[u]
        return self.p.block(AXES[colour][phase], way, step)

    def first(self, own, u, step):
        return pick_block(own.at[u], AXES[UNITS[u][0]][0], self.block(u, 0, step))

    def second(self, e, u, step):
        order = AXES[UNITS[u][0]]
        b = self.block(u, 1, step)
        rest = [a for a in NAT if a != order[0]]
        return self.t1[e, u, :, b] if rest.index(order[1]) == 1 else self.t1[e, u, b]

    def third(self, e, u, step):
        return self.t2[e, u, self.block(u, 2, step)]

    def slot(self, n, iteration):
        e, j = n % STREAMS, n // STREAMS
        step = (j - J0[e]) % 3
        k = iteration + (j - J0[e]) // 3
        par = lax.rem(3 * iteration + j, 2)
        old = 1 - par
        chunk = lambda i: STREAMS * (k - i) + POS[e]
        live = lambda i: (chunk(i) >= 0) & (chunk(i) < CHUNKS)
        new = 1 if step == 0 else 0

        @pl.when(live(new))
        def _():
            self.wait(e, old, 0)

        @pl.when(jnp.logical_not(live(new)) & (live(new + 1) | live(new + 2)))
        def _():
            self.wait(e, old, FROM[1])

        if step == 0:
            @pl.when(live(3))
            def _():
                for u in range(NU):
                    self.done[chunk(3), u] = self.came(e, old, u, 2) + self.third(e, u, 3)

            @pl.when(live(2))
            def _():
                for u in range(NU):
                    self.t2[e, u] = self.came(e, old, u, 1) + self.second(e, u, 3)
                    self.go(e, u, 2, self.third(e, u, 0))

            @pl.when(live(1))
            def _():
                own = self.own(chunk(1))
                for u in range(NU):
                    self.t1[e, u] = self.came(e, old, u, 0) + self.first(own, u, 3)
                    self.go(e, u, 1, self.second(e, u, 0))

            @pl.when(live(0))
            def _():
                self.ready(chunk(0))
                own = self.own(chunk(0))
                for u in range(NU):
                    self.go(e, u, 0, self.first(own, u, 0))
        else:
            @pl.when(live(2))
            def _():
                for u in range(NU):
                    self.go(e, u, 2, self.came(e, old, u, 2) + self.third(e, u, step))

            @pl.when(live(1))
            def _():
                for u in range(NU):
                    self.go(e, u, 1, self.came(e, old, u, 1) + self.second(e, u, step))

            @pl.when(live(0))
            def _():
                own = self.own(chunk(0))
                for u in range(NU):
                    self.go(e, u, 0, self.came(e, old, u, 0) + self.first(own, u, step))

        @pl.when(live(0))
        def _():
            self.send(e, par, 0)

        @pl.when(jnp.logical_not(live(0)) & (live(1) | live(2)))
        def _():
            self.send(e, par, FROM[1])


def tiles_of_layer():
    down = [(3, g, j) for j in range(4) for g in range(4)]
    up = [(2, 0, j) for j in range(16)]
    out = [(1, 0, j) for j in range(4)]
    qkv = [(0, 0, j) for j in range(12)]
    return down + up + out + qkv


TILES = tiles_of_layer()
PLACE_OF = {t: (i // 12, i % 12 // 6, i % 6) for i, t in enumerate(TILES)}


FWD_SEQS = 3
BWD_SEQS = 2
OWN_SLOTS = 8
DRAIN = 3
QKV_W, OUT_W, UP_W, DOWN_W = range(4)
HALF = 2 * D


def step_kernel(x, seed, wq, wo, wu, wd,
                y, rq, ro, ru, rd, hs, qs, ps, os, ms, us, out,
                grads, recv, done, h, qkv, p, o, m, u, e, g, g1, do, acc, vq, vo, vu, vd,
                wsem, asem, gsem, psem, qsem, hsem, ysem, dsend, drecv, fsem, credit, *ring):
    place = Place()
    core = place.core
    partner = place.partner()
    mine = (wq, wo, wu, wd)
    theirs = (rq, ro, ru, rd)
    held = (vq, vo, vu, vd)
    acts = ((h, hs), (qkv, qs), (p, ps), (o, os), (m, ms), (u, us))
    H, QKV, PROB, O, M, U = range(6)
    rows = pl.ds(core * ROWS, ROWS)

    def to_partner(src, dst, send, arrive):
        return pltpu.make_async_remote_copy(src, dst, send, arrive, device_id=partner, device_id_type=MESH)

    def push(k, j):
        return to_partner(mine[k].at[j], theirs[k].at[j], psem.at[k, j], qsem.at[k, j])

    halves = [(UP_W, (slice(None), pl.ds(0, HALF))), (DOWN_W, (pl.ds(0, HALF),)),
              (UP_W, (slice(None), pl.ds(HALF, HALF))), (DOWN_W, (pl.ds(HALF, HALF),))]
    direct = [(QKV_W, ()), (OUT_W, ())] + halves

    def hand(i):
        k, at = direct[i]
        src, dst = mine[k].at[0], held[k]
        if at:
            src, dst = src.at[at], dst.at[at]
        return to_partner(src, dst, hsem.at[0, i], hsem.at[1, i])

    def local_w(k, l, src):
        return pltpu.make_async_copy(src[k].at[lax.rem(l, 2)], held[k], wsem.at[k])

    def fetch_w(k, l, arrives):
        @pl.when(l // 2 == core)
        def _():
            local_w(k, l, mine).start()

        @pl.when(l // 2 != core)
        def _():
            @pl.when(arrives)
            def _():
                push(k, lax.rem(l, 2)).wait_recv()
            local_w(k, l, theirs).start()

    def wait_w(k):
        local_w(k, 0, mine).wait()

    def act(i, l, back):
        vmem, hbm = acts[i]
        return pltpu.make_async_copy(hbm.at[l], vmem, asem.at[i]) if back else pltpu.make_async_copy(vmem, hbm.at[l], asem.at[i])

    def own_slot(chunk):
        return lax.rem(chunk, OWN_SLOTS)

    def cross(chunk):
        q = lax.rem(chunk, 4)
        return to_partner(grads.at[OWN_SLOTS + q], recv.at[q], dsend.at[q], drecv.at[q])

    def ready(chunk):
        q = lax.rem(chunk, 4)
        cross(chunk).wait_recv()
        for unit in range(NU):
            grads[own_slot(chunk), unit] = grads[own_slot(chunk), unit] + recv[q, unit]

        @pl.when(chunk + 4 < CHUNKS)
        def _():
            pl.semaphore_signal(credit.at[q], inc=1, device_id=partner, device_id_type=MESH)

    rings = Rings(place, ring, lambda chunk: grads.at[own_slot(chunk)], ready, done)

    x_in = pltpu.make_async_copy(x.at[rows], h, asem.at[H])
    x_in.start()
    seed_in = pltpu.make_async_copy(seed.at[rows], g, gsem)

    @pl.when(core == 0)
    def _():
        for k in range(4):
            local_w(k, 0, mine).start()
    greet([partner] + [place.neighbour(a, way) for a in NAT for way in (1, -1)])

    @pl.when(core == 0)
    def _():
        for i in range(len(direct)):
            hand(i).start()
        for j in (1, 0):
            for k in range(4):
                push(k, j).start()

    @pl.when(core == 1)
    def _():
        for j in range(2):
            for k in range(4):
                push(k, j).start()
    seed_in.start()
    x_in.wait()

    def layer(l, _):
        handed = (l == 0) & (core == 1)

        def weight(k, parts=()):
            @pl.when(jnp.logical_not(handed))
            def _():
                wait_w(k)

            @pl.when(handed)
            def _():
                for i in parts or (k,):
                    hand(i).wait_recv()

        def again(i):
            @pl.when(l > 0)
            def _():
                act(i, l - 1, False).wait()

        def save(i):
            @pl.when(l < LAYERS - 1)
            def _():
                act(i, l, False).start()

        def next_w(*ks):
            @pl.when(l < LAYERS - 1)
            def _():
                for k in ks:
                    fetch_w(k, l + 1, True)

        again(H)

        @pl.when(l > 0)
        def _():
            h[...] = do[...]
        save(H)
        weight(QKV_W)
        again(QKV)
        hf = h[...].astype(F32)
        qkv[...] = dot((hf * inv_rms(hf)).astype(BF16), vq[...]).astype(BF16)
        save(QKV)
        again(PROB)
        again(O)

        def attend(i, _):
            attention_fwd(i, FWD_SEQS, qkv, p, o)
            return 0

        lax.fori_loop(0, NSEQ // FWD_SEQS, attend, 0)
        save(PROB)
        save(O)
        weight(OUT_W)
        again(M)
        m[...] = (h[...].astype(F32) + dot(o[...], vo[...])).astype(BF16)
        save(M)
        again(U)
        weight(UP_W, (2, 3))

        @pl.when(jnp.logical_not(handed))
        def _():
            wait_w(DOWN_W)

        def mlp(j):
            cols = slice(j * HALF, (j + 1) * HALF)
            mf = m[...].astype(F32)
            c = (mf * inv_rms(mf)).astype(BF16)
            ub = dot(c, vu[:, cols]).astype(BF16)
            u[:, cols] = ub
            eb = gelu(ub.astype(F32)).astype(BF16)
            e[:, cols] = eb
            return dot(eb, vd[cols, :])

        acc[...] = m[...].astype(F32) + mlp(0)
        next_w(QKV_W, OUT_W)

        @pl.when(handed)
        def _():
            hand(4).wait_recv()
            hand(5).wait_recv()
        do[...] = (acc[...] + mlp(1)).astype(BF16)
        save(U)
        next_w(UP_W, DOWN_W)
        return 0

    lax.fori_loop(0, LAYERS, layer, 0)
    y_here = pltpu.make_async_copy(do, y.at[rows], ysem.at[0])
    y_there = to_partner(do, y.at[rows], ysem.at[1], ysem.at[2])
    y_here.start()
    y_there.start()

    def free(chunk):
        @pl.when(chunk >= 4)
        def _():
            cross(chunk).wait_send()

    def put(base, tile, value):
        q, half, unit = PLACE_OF[tile]
        index = jnp.where(core == half, own_slot(base + q), OWN_SLOTS + q)
        grads[index, unit] = value.reshape((4, 4, 4) + TILE)

    def ship(chunk):
        @pl.when(chunk >= 4)
        def _():
            pl.semaphore_wait(credit.at[lax.rem(chunk, 4)], 1)
        cross(chunk).start()

    def down_grad(base):
        free(base)
        free(base + 1)
        for half in range(2):
            w = dot_first(e[...], g[:, half * 256:half * 256 + 256]).reshape((64, 4, 8, 256))
            for j in range(2):
                for rg in range(4):
                    put(base, (DOWN_W, rg, 2 * half + j), w[:, rg, :, j * LN:j * LN + LN])
        ship(base)

    def gelu_part(j):
        cols = slice(j * D, (j + 1) * D)
        de = dot_last(g[...], vd[cols, :])
        ej, slope = gelu_and_slope(u[:, cols].astype(F32))
        e[:, cols] = ej.astype(BF16)
        u[:, cols] = (slope * de).astype(BF16)

    def wide_grad(base, array, a, b, parts):
        for part in range(parts):
            w = dot_first(a, b[:, part * D:part * D + D]).reshape((64, 8, D))
            for j in range(4):
                put(base, (array, 0, 4 * part + j), w[:, :, j * LN:j * LN + LN])

    seed_in.wait()
    down_grad(0)
    for j in range(4):
        gelu_part(j)
    y_here.wait()
    y_there.wait_send()

    def iteration(it, _):
        l = LAYERS - 1 - it
        more = it < LAYERS - 1
        base = 4 * it

        def loaded(acts_of, w=None):
            @pl.when(it > 0)
            def _():
                for i in acts_of:
                    act(i, l, True).wait()
                if w is not None:
                    wait_w(w)

        def after(acts_of, *ws):
            @pl.when(more)
            def _():
                for k in ws:
                    fetch_w(k, l - 1, l == 1)
                for i in acts_of:
                    act(i, l - 1, True).start()

        def piece(n):
            if n == 0:
                loaded((M,))
                free(base + 2)
                mf = m[...].astype(F32)
                wide_grad(base, UP_W, (mf * inv_rms(mf)).astype(BF16), u, 4)
                ship(base + 1)
            elif n == 1:
                loaded((), UP_W)
                dc = dot_last(u[...], vu[...])
                g1[...] = (g[...].astype(F32) + rms_bwd(m[...].astype(F32), dc)).astype(BF16)
                after((U, M), UP_W, DOWN_W)
            elif n == 2:
                loaded((O,), OUT_W)
                do[...] = dot_last(g1[...], vo[...]).astype(BF16)
                wide_grad(base, OUT_W, o[...], g1, 1)
                ship(base + 2)
                after((O,), OUT_W)
            elif n in (3, 4, 5):
                if n == 3:
                    loaded((PROB, QKV))
                attention_bwd(n - 3, BWD_SEQS, qkv, p, do)
                if n == 5:
                    after((PROB,))
            elif n == 6:
                loaded((H,), QKV_W)
                da = dot_last(qkv[...], vq[...])
                g[...] = (g1[...].astype(F32) + rms_bwd(h[...].astype(F32), da)).astype(BF16)
                after((), QKV_W)
            elif n == 7:
                free(base + 3)
                hf = h[...].astype(F32)
                wide_grad(base, QKV_W, (hf * inv_rms(hf)).astype(BF16), qkv, 3)
                ship(base + 3)
                after((H, QKV))
            elif n in (8, 9):
                @pl.when(more)
                def _():
                    if n == 8:
                        act(U, l - 1, True).wait()
                        wait_w(DOWN_W)
                    for j in range(2):
                        gelu_part(2 * (n - 8) + j)
            elif n == 10:
                @pl.when(more)
                def _():
                    down_grad(base + 4)

        for n in range(12):
            rings.slot(n, it)
            if n < 11:
                @pl.when(it < LAYERS)
                def _():
                    piece(n)
        return 0

    lax.fori_loop(0, LAYERS + DRAIN, iteration, 0)

    for q in range(4):
        cross(CHUNKS - 4 + q).wait_send()
    last = to_partner(done.at[pl.ds(8 * core, 8)], out.at[core], fsem.at[0], fsem.at[1])
    last.start()
    out[core] = done[pl.ds(8 * (1 - core), 8)]
    for j in range(2):
        for k in range(4):
            push(k, j).wait_send()

    @pl.when(core == 0)
    def _():
        for i in range(len(direct)):
            hand(i).wait_send()
    y_there.wait_recv()
    last.wait_send()
    last.wait_recv()


def train_step(x, seed, weights):
    anywhere = pl.BlockSpec(memory_space=pl.ANY)
    vmem = pl.BlockSpec(memory_space=pltpu.VMEM)
    act = lambda cols, dt=BF16: pltpu.VMEM((ROWS, cols), dt)
    saved = lambda cols, dt=BF16: jax.ShapeDtypeStruct((LAYERS - 1, ROWS, cols), dt)
    outs = pl.pallas_call(
        step_kernel,
        name="step",
        out_shape=[jax.ShapeDtypeStruct((2 * ROWS, D), BF16)] + [jax.ShapeDtypeStruct((2,) + s, BF16) for s in W_SHAPES]
        + [saved(D), saved(3 * D), saved(2 * D, F32), saved(D), saved(D), saved(4 * D)]
        + [jax.ShapeDtypeStruct((2, 8, NU) + TILE, F32)],
        in_specs=[anywhere] * 6,
        out_specs=[anywhere] * 11 + [vmem],
        scratch_shapes=[
            pltpu.VMEM((OWN_SLOTS + 4, NU, 4, 4, 4) + TILE, F32),
            pltpu.VMEM((4, NU, 4, 4, 4) + TILE, F32),
            pltpu.VMEM((CHUNKS, NU) + TILE, F32),
            act(D), act(3 * D), act(2 * D, F32), act(D), act(D), act(4 * D), act(4 * D), act(D), act(D), act(D), act(D, F32),
        ] + [pltpu.VMEM(s, BF16) for s in W_SHAPES] + [
            pltpu.SemaphoreType.DMA((4,)), pltpu.SemaphoreType.DMA((6,)), pltpu.SemaphoreType.DMA,
            pltpu.SemaphoreType.DMA((4, 2)), pltpu.SemaphoreType.DMA((4, 2)), pltpu.SemaphoreType.DMA((2, 6)),
            pltpu.SemaphoreType.DMA((3,)),
            pltpu.SemaphoreType.DMA((4,)), pltpu.SemaphoreType.DMA((4,)), pltpu.SemaphoreType.DMA((2,)),
            pltpu.SemaphoreType.REGULAR((4,)),
        ] + ring_scratch(),
        compiler_params=pltpu.CompilerParams(collective_id=1, has_side_effects=True, vmem_limit_bytes=67043328),
    )(x, seed, *weights)
    return outs[0], outs[-1]


def finish_kernel(y_in, sums, y, gq, go, gu, gd, buf, in_sem, out_sem):
    parts = buf.shape[0]
    move = lambda i, into: (pltpu.make_async_copy(y_in.at[i], buf.at[i], in_sem.at[i]) if into
                            else pltpu.make_async_copy(buf.at[i], y.at[i], out_sem.at[i]))
    for i in range(parts):
        move(i, True).start()
    outs = (gq, go, gu, gd)
    for layer in range(2):
        for tile in TILES:
            array, rg, col = tile
            q, half, unit = PLACE_OF[tile]
            outs[array][layer, rg * 8:rg * 8 + 8, col * LN:col * LN + LN] = sums[half, 4 * (1 - layer) + q, unit]
    for i in range(parts):
        move(i, True).wait()
        move(i, False).start()
    for i in range(parts):
        move(i, False).wait()


def finish(y, sums, parts=4):
    anywhere = pl.BlockSpec(memory_space=pl.ANY)
    vmem = pl.BlockSpec(memory_space=pltpu.VMEM)
    shape = (parts, 2 * ROWS // parts, D)
    return pl.pallas_call(
        finish_kernel,
        name="finish",
        out_shape=[jax.ShapeDtypeStruct(shape, BF16)]
        + [jax.ShapeDtypeStruct(s, F32) for s in ((2, 8, 3 * D), (2, 8, D), (2, 8, 4 * D), (2, 32, D))],
        in_specs=[anywhere, vmem],
        out_specs=[anywhere] + [vmem] * 4,
        scratch_shapes=[pltpu.VMEM(shape, BF16), pltpu.SemaphoreType.DMA((parts,)), pltpu.SemaphoreType.DMA((parts,))],
    )(y.reshape(shape), sums)


def solution(mesh):
    def step(x_in, seed_grad, w_qkv, w_out, w_up, w_down):
        shape = x_in.shape
        weights = (w_qkv, w_out, w_up, w_down)
        y, sums = train_step(x_in.reshape(2 * ROWS, D), seed_grad.reshape(2 * ROWS, D), weights)
        y, *grads = finish(y, sums)
        return y.reshape(shape), *grads

    act, weight, grad = P(None, "dp"), P("pp"), P("pp", "dp")
    return jax.shard_map(
        step,
        mesh=mesh,
        in_specs=(act, act, weight, weight, weight, weight),
        out_specs=(act, grad, grad, grad, grad),
        check_vma=False,
    )
```

```python
import functools
import math

import jax
import jax.numpy as jnp
from jax import lax
from jax.experimental import pallas as pl
from jax.experimental.pallas import tpu as pltpu
from jax.sharding import PartitionSpec as P

F32 = jnp.float32
BF16 = jnp.bfloat16
MESH = pl.DeviceIdType.MESH

D = 512
HD = 64
LN = 128
TILE = (8, LN)
QUAD = 4
PLANE = (QUAD, QUAD)
CUBE = PLANE + (QUAD,)
NU = 6
SEQ = LN
NSEQ = 6
ROWS = NSEQ * SEQ
LAYERS = 4
EPS = 1e-6
GELU_C1 = math.sqrt(2.0 / math.pi)
GELU_C2 = GELU_C1 * 0.044715
EXP2_SCALE = HD ** -0.5 * math.log2(math.e)
W_SHAPES = ((D, 3 * D), (D, D), (D, QUAD * D), (QUAD * D, D))
LAST = (((1,), (1,)), ((), ()))
FIRST = (((0,), (0,)), ((), ()))


def dot(a, b):
    return jnp.dot(a, b, preferred_element_type=F32)


def dot_last(a, b):
    return lax.dot_general(a, b, LAST, preferred_element_type=F32)


def dot_first(a, b):
    return lax.dot_general(a, b, FIRST, preferred_element_type=F32)


def inv_rms(h):
    return lax.rsqrt(jnp.mean(h * h, axis=-1, keepdims=True) + EPS)


def rms_bwd(h, g):
    ir = inv_rms(h)
    n = h * ir
    return ir * (g - n * jnp.mean(g * n, axis=-1, keepdims=True))


def gelu(u):
    t = jnp.tanh(u * (GELU_C1 + GELU_C2 * (u * u)))
    return u * (0.5 * t + 0.5)


def gelu_slope(u):
    a = GELU_C2 * (u * u)
    t = jnp.tanh(u * (a + GELU_C1))
    half = 0.5 * t + 0.5
    return half + u * half * (1.0 - t) * (3.0 * a + GELU_C1)


def block_diag(x):
    first = lax.broadcasted_iota(jnp.int32, (SEQ, 2 * HD), 1) < HD
    zero = jnp.zeros_like(x)
    return jnp.concatenate([jnp.where(first, x, zero), jnp.where(first, zero, x)], axis=0)


def units_of(step, n_seqs):
    return [(pl.ds(pl.multiple_of((step * n_seqs + n) * SEQ, SEQ), SEQ), pair) for n in range(n_seqs) for pair in range(QUAD)]


def attention_fwd(step, n_seqs, qkv, p_out, o_out):
    key = lax.broadcasted_iota(jnp.int32, (SEQ, SEQ), 0)
    query = lax.broadcasted_iota(jnp.int32, (SEQ, SEQ), 1)
    allowed = key <= query
    units = units_of(step, n_seqs)

    def scores(rows, pair):
        c = pair * LN
        return dot_last(qkv[rows, D + c:D + c + LN], block_diag(qkv[rows, c:c + LN]))

    ahead = 2
    pending = [scores(*u) for u in units[:ahead]]
    for i, (rows, pair) in enumerate(units):
        if i + ahead < len(units):
            pending.append(scores(*units[i + ahead]))
        s = pending[i]
        c = pair * LN
        probs = []
        for head in range(2):
            sh = jnp.where(allowed, s[:, head * LN:head * LN + LN], -1e30)
            e = jnp.exp2((sh - jnp.max(sh, axis=0, keepdims=True)) * EXP2_SCALE)
            p = e * (1.0 / jnp.sum(e, axis=0, keepdims=True))
            p_out[rows, 2 * c + head * LN:2 * c + head * LN + LN] = p
            probs.append(p.astype(BF16))
        v = qkv[rows, 2 * D + c:2 * D + c + LN]
        o_out[rows, c:c + LN] = dot_first(jnp.concatenate(probs, axis=0), block_diag(v)).astype(BF16)


def attention_bwd(step, n_seqs, qkv, p_in, do):
    units = units_of(step, n_seqs)

    def first(rows, pair):
        c = pair * LN
        d = block_diag(do[rows, c:c + LN])
        return d, dot_last(qkv[rows, 2 * D + c:2 * D + c + LN], d)

    ahead = 2
    pending = [first(*u) for u in units[:ahead]]
    for i, (rows, pair) in enumerate(units):
        if i + ahead < len(units):
            pending.append(first(*units[i + ahead]))
        d, dp = pending[i]
        c = pair * LN
        q = qkv[rows, c:c + LN]
        k = qkv[rows, D + c:D + c + LN]
        p = p_in[rows, 2 * c:2 * c + 256]
        dv = dot(p.astype(BF16), d).astype(BF16)
        pd = p * dp
        ds = ((pd - p * jnp.sum(pd, axis=0, keepdims=True)) * HD ** -0.5).astype(BF16)
        dk = dot(ds, block_diag(q)).astype(BF16)
        dq = dot_first(jnp.concatenate([ds[:, :LN], ds[:, LN:]], axis=0), block_diag(k)).astype(BF16)
        qkv[rows, c:c + LN] = dq
        qkv[rows, D + c:D + c + LN] = dk
        qkv[rows, 2 * D + c:2 * D + c + LN] = dv


AXES = (("x", "y", "z"), ("y", "z", "x"), ("z", "x", "y"))
NAT = ("z", "y", "x")
STRIDE = {"x": 1, "y": 4, "z": 16}
UNITS = [(colour, way) for colour in range(3) for way in (1, -1)]


class Place:
    def __init__(self):
        self.core = lax.axis_index("pp")
        self.dp = lax.axis_index("dp")
        self.at = {"x": lax.rem(self.dp, QUAD), "y": lax.rem(self.dp // QUAD, QUAD), "z": self.dp // 16}

    def neighbour(self, axis, way):
        c = self.at[axis]
        return (self.core, self.dp + (lax.rem(c + way + QUAD, QUAD) - c) * STRIDE[axis])

    def partner(self):
        return (1 - self.core, self.dp)

    def block(self, axis, way, step):
        return lax.rem(self.at[axis] - way * (1 + step) + 8, QUAD)


def greet(peers):
    barrier = pltpu.get_barrier_semaphore()
    for p in peers:
        pl.semaphore_signal(barrier, inc=1, device_id=p, device_id_type=MESH)
    pl.semaphore_wait(barrier, len(peers))


CHUNKS = 16
PERIOD = 3
STREAMS = 4
SLOTS = PERIOD * CHUNKS
HOP = (16, 4, 1)
FROM = (0, 16, 20)
LINK = 21


def ring_scratch():
    dma = pltpu.SemaphoreType.DMA
    return [
        pltpu.VMEM((STREAMS, NU, LINK) + TILE, F32), pltpu.VMEM((STREAMS, 2, NU, LINK) + TILE, F32),
        pltpu.VMEM((STREAMS, NU) + PLANE + TILE, F32), pltpu.VMEM((STREAMS, NU, 4) + TILE, F32),
        pltpu.VMEM((STREAMS, 3, NU, 4) + TILE, F32), pltpu.VMEM((2, STREAMS, 3, NU) + TILE, F32),
        dma((STREAMS,)), dma((STREAMS, 2)), dma((3, STREAMS)), dma((3, STREAMS)),
    ]


def pick_block(ref, axis, b):
    return {"z": lambda: ref[b], "y": lambda: ref[:, b], "x": lambda: ref[:, :, b]}[axis]()


class Rings:
    def __init__(self, place, scratch, own, ready, done):
        self.p, self.own, self.ready, self.done = place, own, ready, done
        self.sent, self.got, self.t1, self.t2, self.d2, self.d3, self.ss, self.rs, self.ds, self.dr = scratch
        self.sent[:, :, FROM[1]:] = jnp.zeros((STREAMS, NU, LINK - FROM[1]) + TILE, F32)

    def links(self, e, par, link, lo):
        tiles = pl.ds(lo, LINK - lo)
        axis, way = UNITS[0 if link is None else link]
        at = slice(None) if link is None else link
        return pltpu.make_async_remote_copy(self.sent.at[e, at, tiles], self.got.at[e, par, at, tiles], self.ss.at[e], self.rs.at[e, par],
                                            device_id=self.p.neighbour("xyz"[axis], way), device_id_type=MESH)

    def wait(self, e, par, lo):
        c = self.links(e, par, None, lo)
        c.wait_send()
        c.wait_recv()

    def send(self, e, par, lo):
        for link in range(NU):
            self.links(e, par, link, lo).start()

    def link(self, u, phase):
        return (u + 2 * phase) % NU

    def came(self, e, par, u, phase):
        lo = FROM[phase]
        v = self.got[e, par, self.link(u, phase), lo:lo + HOP[phase]]
        return v.reshape((PLANE, PLANE[1:], ())[phase] + TILE)

    def go(self, e, u, phase, value):
        lo = FROM[phase]
        self.sent[e, self.link(u, phase), lo:lo + HOP[phase]] = value.reshape((HOP[phase],) + TILE)

    def block(self, u, phase, step):
        colour, way = UNITS[u]
        return self.p.block(AXES[colour][phase], way, step)

    def first(self, own, u, step):
        return pick_block(own.at[u], AXES[UNITS[u][0]][0], self.block(u, 0, step))

    def second_ref(self, e, u, b):
        order = AXES[UNITS[u][0]]
        rest = [a for a in NAT if a != order[0]]
        return self.t1.at[(e, u, slice(None), b) if rest.index(order[1]) == 1 else (e, u, b)]

    def second(self, e, u, step):
        return self.second_ref(e, u, self.block(u, 1, step))[...]

    def third(self, e, u, step):
        return self.t2[e, u, self.block(u, 2, step)]

    def straight(self, e, kind, u, j):
        phase = 1 if kind == 0 else 2
        axis = AXES[UNITS[u][0]][phase]
        b = lax.rem(self.p.at[axis] + j, QUAD)
        src = self.second_ref(e, u, b) if kind == 0 else self.t2.at[e, u, b]
        dst = self.landing(e, kind).at[j - 1, u]
        return pltpu.make_async_remote_copy(src, dst, self.ds.at[kind, e], self.dr.at[kind, e],
                                            device_id=self.p.neighbour(axis, j), device_id_type=MESH)

    def landing(self, e, kind):
        return self.d2.at[e] if kind == 0 else self.d3.at[kind - 1, e]

    def go_straight(self, e, kind):
        for j in (1, 3, 2):
            for u in range(NU):
                self.straight(e, kind, u, j).start()

    def wait_straight(self, e, kind):
        at = self.landing(e, kind)
        c = pltpu.make_async_remote_copy(at, at, self.ds.at[kind, e], self.dr.at[kind, e],
                                         device_id=self.p.neighbour("x", 1), device_id_type=MESH)
        c.wait_send()
        c.wait_recv()

    def sum_straight(self, e, kind, u):
        at = self.landing(e, kind)
        return at[0, u] + at[1, u] + at[2, u]

    def slot(self, s, step, drain=False):
        e = lax.rem(s, STREAMS)
        par = lax.rem(s // STREAMS, 2)
        old = 1 - par
        since = s - STREAMS * step
        chunk = lambda i: since // PERIOD - STREAMS * i
        live = lambda i: (since >= PERIOD * STREAMS * i) & (chunk(i) < CHUNKS)
        early = lambda i: chunk(i) < CHUNKS - 2 * STREAMS
        not_late = lambda i: chunk(i) < CHUNKS - STREAMS
        if not drain:
            early = not_late = lambda i: True
        both = lambda a, b: a if b is True else a & b
        ring1 = both(live(1), not_late(1))
        ring2 = both(live(2), early(2))
        late = live(1) & jnp.logical_not(not_late(1)) if drain else None
        middle = live(2) & not_late(2) & jnp.logical_not(early(2)) if drain else None
        if step == 0:
            was, more = live(1), both(live(2), not_late(2)) | both(live(3), early(3))
        else:
            was, more = live(0), ring1 | ring2

        @pl.when(was)
        def _():
            self.wait(e, old, 0)

        @pl.when(jnp.logical_not(was) & more)
        def _():
            self.wait(e, old, FROM[1])

        if step == 0:
            @pl.when(both(live(3), early(3)))
            def _():
                for u in range(NU):
                    self.done[chunk(3), u] = self.came(e, old, u, 2) + self.third(e, u, 3)

            @pl.when(both(live(2), not_late(2)))
            def _():
                for u in range(NU):
                    self.t2[e, u] = self.came(e, old, u, 1) + self.second(e, u, 3)
                    self.go(e, u, 2, self.third(e, u, 0))

            @pl.when(live(1))
            def _():
                own = self.own(chunk(1))
                for u in range(NU):
                    self.t1[e, u] = self.came(e, old, u, 0) + self.first(own, u, 3)
                    self.go(e, u, 1, self.second(e, u, 0))

            @pl.when(live(0))
            def _():
                self.ready(chunk(0))
                own = self.own(chunk(0))
                for u in range(NU):
                    self.go(e, u, 0, self.first(own, u, 0))
        else:
            @pl.when(ring2)
            def _():
                for u in range(NU):
                    self.go(e, u, 2, self.came(e, old, u, 2) + self.third(e, u, step))

            if drain and step == 1:
                @pl.when(middle)
                def _():
                    self.wait_straight(e, 2)
                    for u in range(NU):
                        self.done[chunk(2), u] = self.sum_straight(e, 2, u) + self.third(e, u, 3)

            @pl.when(ring1)
            def _():
                for u in range(NU):
                    self.go(e, u, 1, self.came(e, old, u, 1) + self.second(e, u, step))

            if drain:
                @pl.when(late)
                def _():
                    self.wait_straight(e, step - 1)
                    for u in range(NU):
                        if step == 1:
                            self.t2[e, u] = self.sum_straight(e, 0, u) + self.second(e, u, 3)
                        else:
                            self.done[chunk(1), u] = self.sum_straight(e, 1, u) + self.third(e, u, 3)

            @pl.when(live(0))
            def _():
                own = self.own(chunk(0))
                for u in range(NU):
                    self.go(e, u, 0, self.came(e, old, u, 0) + self.first(own, u, step))

        @pl.when(live(0))
        def _():
            self.send(e, par, 0)

        @pl.when(jnp.logical_not(live(0)) & (ring1 | ring2))
        def _():
            self.send(e, par, FROM[1])

        if drain and step < 2:
            @pl.when(late)
            def _():
                self.go_straight(e, step)

        if drain and step == 0:
            @pl.when(middle)
            def _():
                self.go_straight(e, 2)

    def step_of(self, s):
        return s * (STREAMS % PERIOD) % PERIOD if isinstance(s, int) else lax.rem(s * (STREAMS % PERIOD), PERIOD)

    def drain(self, start):
        def one(s, _):
            at = self.step_of(s)
            for step in range(PERIOD):
                @pl.when(at == step)
                def _():
                    self.slot(s, step, True)
            return 0

        lax.fori_loop(start, SLOTS - PERIOD + 5 * STREAMS + 1, one, 0)


def tiles_of_layer():
    down = [(3, g, j) for j in range(QUAD) for g in range(QUAD)]
    up = [(2, 0, j) for j in range(16)]
    out = [(1, 0, j) for j in range(QUAD)]
    qkv = [(0, 0, j) for j in range(12)]
    return down + up + out + qkv


TILES = tiles_of_layer()
PLACE_OF = {t: (i // 12, i % 12 // 6, i % 6) for i, t in enumerate(TILES)}


FWD_SEQS = 3
BWD_SEQS = 2
OWN_SLOTS = 6
LEAD = 2
QKV_W, OUT_W, UP_W, DOWN_W = range(4)
HALF = 2 * D
PIECES = [(QKV_W, ()), (OUT_W, ()), (UP_W, (slice(None), pl.ds(0, HALF))), (DOWN_W, (pl.ds(0, HALF),)),
          (UP_W, (slice(None), pl.ds(HALF, HALF))), (DOWN_W, (pl.ds(HALF, HALF),))]
ALL = range(len(PIECES))
QKV_P, OUT_P, UP_P, DOWN_P = (0,), (1,), (2, 4), (3, 5)


def step_kernel(x, seed, wq, wo, wu, wd,
                y, rq, ro, ru, rd, hs, qs, ps, os, ms, us, es, out,
                grads, recv, done, h, qkv, p, o, m, u, e, g, g1, do, vq, vo, vu, vd,
                wsem, asem, gsem, psem, qsem, hsem, ysem, dsend, drecv, fsem, credit, wfree, *ring):
    place = Place()
    core = place.core
    partner = place.partner()
    mine = (wq, wo, wu, wd)
    theirs = (rq, ro, ru, rd)
    held = (vq, vo, vu, vd)
    acts = ((h, hs), (qkv, qs), (p, ps), (o, os), (m, ms), (u, us), (e, es))
    H, QKV, PROB, O, M, U, E = range(7)
    rows = pl.ds(core * ROWS, ROWS)

    def to_partner(src, dst, send, arrive):
        return pltpu.make_async_remote_copy(src, dst, send, arrive, device_id=partner, device_id_type=MESH)

    def piece_of(ref, i):
        at = PIECES[i][1]
        return ref.at[at] if at else ref

    def push(i, j):
        k = PIECES[i][0]
        return to_partner(piece_of(mine[k].at[j], i), piece_of(theirs[k].at[j], i), psem.at[i, j], qsem.at[i, j])

    def hand(i, l):
        k = PIECES[i][0]
        return to_partner(piece_of(mine[k].at[l], i), piece_of(held[k], i), hsem.at[0, i], hsem.at[1, i])

    def local_w(i, l, src):
        k = PIECES[i][0]
        return pltpu.make_async_copy(piece_of(src[k].at[lax.rem(l, 2)], i), piece_of(held[k], i), wsem.at[i])

    def fetch_w(i, l, arrives):
        @pl.when(l // 2 == core)
        def _():
            local_w(i, l, mine).start()

        @pl.when(l // 2 != core)
        def _():
            @pl.when(arrives)
            def _():
                push(i, lax.rem(l, 2)).wait_recv()
            local_w(i, l, theirs).start()

    def wait_w(*pieces):
        for i in pieces:
            local_w(i, 0, mine).wait()

    def act(i, l, back):
        vmem, hbm = acts[i]
        return pltpu.make_async_copy(hbm.at[l], vmem, asem.at[i]) if back else pltpu.make_async_copy(vmem, hbm.at[l], asem.at[i])

    def own_slot(chunk):
        return lax.rem(chunk, OWN_SLOTS)

    def cross(chunk):
        q = lax.rem(chunk, QUAD)
        return to_partner(grads.at[OWN_SLOTS + q], recv.at[q], dsend.at[q], drecv.at[q])

    def ready(chunk):
        q = lax.rem(chunk, QUAD)
        cross(chunk).wait_recv()
        for unit in range(NU):
            grads[own_slot(chunk), unit] = grads[own_slot(chunk), unit] + recv[q, unit]

        @pl.when(chunk + QUAD < CHUNKS)
        def _():
            pl.semaphore_signal(credit.at[q], inc=1, device_id=partner, device_id_type=MESH)

    rings = Rings(place, ring, lambda chunk: grads.at[own_slot(chunk)], ready, done)

    x_in = pltpu.make_async_copy(x.at[rows], h, asem.at[H])
    x_in.start()
    seed_in = pltpu.make_async_copy(seed.at[rows], g, gsem)

    @pl.when(core == 0)
    def _():
        for i in ALL:
            local_w(i, 0, mine).start()
    greet([partner] + [place.neighbour(a, way) for a in NAT for way in (1, -1, 2)])

    @pl.when(core == 0)
    def _():
        for i in ALL:
            hand(i, 0).start()

    @pl.when(core == 1)
    def _():
        for j in range(2):
            for i in ALL:
                push(i, j).start()
    seed_in.start()
    x_in.wait()

    def layer(l, _):
        handed = (l < 2) & (core == 1)

        def weight(*pieces):
            @pl.when(jnp.logical_not(handed))
            def _():
                wait_w(*pieces)

            @pl.when(handed)
            def _():
                for i in pieces:
                    hand(i, 0).wait_recv()

        def used(group):
            @pl.when((l == 0) & (core == 1))
            def _():
                pl.semaphore_signal(wfree.at[group], inc=1, device_id=partner, device_id_type=MESH)

        def hand_on(at, group, *pieces):
            @pl.when((l == at) & (core == 0))
            def _():
                pl.semaphore_wait(wfree.at[group], 1)
                for i in pieces:
                    hand(i, 0).wait_send()
                    hand(i, 1).start()

        def again(i):
            @pl.when(l > 0)
            def _():
                act(i, l - 1, False).wait()

        def save(i):
            @pl.when(l < LAYERS - 1)
            def _():
                act(i, l, False).start()

        def next_w(when, to, *pieces):
            @pl.when(when)
            def _():
                for i in pieces:
                    fetch_w(i, to, True)

        more = l < LAYERS - 1
        again(H)

        @pl.when(l > 0)
        def _():
            h[...] = do[...]
        save(H)
        weight(0)
        again(QKV)
        hf = h[...].astype(F32)
        qkv[...] = dot((hf * inv_rms(hf)).astype(BF16), vq[...]).astype(BF16)
        used(0)
        hand_on(1, 2, 2, 3)
        save(QKV)
        again(PROB)
        again(O)

        def attend(i, _):
            attention_fwd(i, FWD_SEQS, qkv, p, o)
            return 0

        lax.fori_loop(0, NSEQ // FWD_SEQS, attend, 0)
        save(PROB)
        save(O)
        hand_on(1, 3, 4, 5)
        weight(1)
        again(M)
        m[...] = (h[...].astype(F32) + dot(o[...], vo[...])).astype(BF16)
        used(1)
        save(M)
        again(U)
        again(E)
        weight(2, 3)

        def mlp(j):
            cols = slice(j * HALF, (j + 1) * HALF)
            mf = m[...].astype(F32)
            c = (mf * inv_rms(mf)).astype(BF16)
            ub = dot(c, vu[:, cols]).astype(BF16)
            u[:, cols] = ub
            eb = gelu(ub.astype(F32)).astype(BF16)
            e[:, cols] = eb
            return dot(eb, vd[cols, :])

        half_way = m[...].astype(F32) + mlp(0)
        for unit in range(NU):
            for col in range(QUAD):
                grads[0, unit, :, :, col] = half_way[unit * SEQ:unit * SEQ + SEQ, col * LN:col * LN + LN].reshape(PLANE + TILE)
        used(2)
        mine_next = more & jnp.logical_or(l > 0, core == 0)
        next_w(mine_next, l + 1, 0, 1)
        weight(4, 5)
        rest = mlp(1)
        for unit in range(NU):
            part = pl.ds(unit * SEQ, SEQ)
            for col in range(QUAD):
                cols = slice(col * LN, col * LN + LN)
                do[part, cols] = (grads[0, unit, :, :, col].reshape((SEQ, LN)) + rest[unit * SEQ:unit * SEQ + SEQ, cols]).astype(BF16)
        used(3)
        hand_on(0, 0, 0)
        hand_on(0, 1, 1)
        next_w(mine_next, l + 1, 2, 3, 4, 5)

        @pl.when((l == 1) & (core == 0))
        def _():
            for j in (1, 0):
                for i in ALL:
                    push(i, j).start()
        save(U)
        save(E)
        return 0

    lax.fori_loop(0, LAYERS, layer, 0)
    y_here = pltpu.make_async_copy(do, y.at[rows], ysem.at[0])
    y_there = to_partner(do, y.at[rows], ysem.at[1], ysem.at[2])
    y_here.start()
    y_there.start()

    def free(chunk):
        @pl.when(chunk >= QUAD)
        def _():
            cross(chunk).wait_send()

    def put(base, tile, value):
        q, half, unit = PLACE_OF[tile]
        index = jnp.where(core == half, own_slot(base + q), OWN_SLOTS + q)
        grads[index, unit] = value.reshape(CUBE + TILE)

    def ship(chunk):
        @pl.when(chunk >= QUAD)
        def _():
            pl.semaphore_wait(credit.at[lax.rem(chunk, QUAD)], 1)
        cross(chunk).start()

    def down_grad(base):
        free(base)
        free(base + 1)
        for half in range(2):
            w = dot_first(e[...], g[:, half * 256:half * 256 + 256]).reshape((64, 4, 8, 256))
            for j in range(2):
                for rg in range(QUAD):
                    put(base, (DOWN_W, rg, 2 * half + j), w[:, rg, :, j * LN:j * LN + LN])
        ship(base)

    def gelu_part(lo, hi):
        de = dot_last(g[...], vd[lo:hi, :])
        u[:, lo:hi] = (gelu_slope(u[:, lo:hi].astype(F32)) * de).astype(BF16)

    def wide_grad(base, array, a, b, parts):
        for part in parts:
            w = dot_first(a, b[:, part * D:part * D + D]).reshape((64, 8, D))
            for j in range(QUAD):
                put(base, (array, 0, QUAD * part + j), w[:, :, j * LN:j * LN + LN])

    seed_in.wait()
    down_grad(0)
    act(E, LAYERS - 2, True).start()
    y_here.wait()
    y_there.wait_send()

    def iteration(it, _):
        l = LAYERS - 1 - it
        more = it < LAYERS - 1
        base = 4 * it

        def loaded(acts_of, pieces=()):
            @pl.when(it > 0)
            def _():
                for i in acts_of:
                    act(i, l, True).wait()
                wait_w(*pieces)

        def after(acts_of, pieces=()):
            @pl.when(more)
            def _():
                for i in pieces:
                    fetch_w(i, l - 1, l <= 2)
                for i in acts_of:
                    act(i, l - 1, True).start()

        def piece(n):
            if n == 0:
                loaded((U,), DOWN_P)
                gelu_part(0, 3 * 256)
            elif n == 1:
                gelu_part(3 * 256, 3 * D)
            elif n == 2:
                gelu_part(3 * D, QUAD * D)
                after((), DOWN_P)
                loaded((M,))
                mf = m[...].astype(F32)
                g1[...] = (mf * inv_rms(mf)).astype(BF16)
                wide_grad(base, UP_W, g1[...], u, (0,))
            elif n == 3:
                free(base + 2)
                wide_grad(base, UP_W, g1[...], u, (1, 2, 3))
                ship(base + 1)
            elif n == 4:
                loaded((), UP_P)
                dc = dot_last(u[...], vu[...])
                g1[...] = (g[...].astype(F32) + rms_bwd(m[...].astype(F32), dc)).astype(BF16)
                after((U, M), UP_P)
            elif n == 5:
                loaded((O,), OUT_P)
                do[...] = dot_last(g1[...], vo[...]).astype(BF16)
                wide_grad(base, OUT_W, o[...], g1, (0,))
                ship(base + 2)
                after((O,), OUT_P)
            elif n in (6, 7, 8):
                if n == 6:
                    loaded((PROB, QKV))
                attention_bwd(n - 6, BWD_SEQS, qkv, p, do)
                if n == 8:
                    after((PROB,))
            elif n == 9:
                loaded((H,))
                free(base + 3)
                hf = h[...].astype(F32)
                wide_grad(base, QKV_W, (hf * inv_rms(hf)).astype(BF16), qkv, (0, 1, 2))
                ship(base + 3)
            elif n == 10:
                loaded((), QKV_P)
                da = dot_last(qkv[...], vq[...])
                g[...] = (g1[...].astype(F32) + rms_bwd(h[...].astype(F32), da)).astype(BF16)
                after((H, QKV), QKV_P)
            else:
                @pl.when(more)
                def _():
                    act(E, l - 1, True).wait()
                    down_grad(base + QUAD)

                @pl.when(l > 1)
                def _():
                    act(E, l - 2, True).start()

        for n in range(12):
            s = 12 * it + n - LEAD
            step = rings.step_of(n + PERIOD - LEAD)
            if n < LEAD:
                @pl.when(it > 0)
                def _():
                    rings.slot(s, step)
            else:
                rings.slot(s, step)
            piece(n)
        return 0

    lax.fori_loop(0, LAYERS, iteration, 0)
    rings.drain(SLOTS - LEAD)

    for q in range(QUAD):
        cross(CHUNKS - 4 + q).wait_send()
    last = to_partner(done.at[pl.ds(8 * core, 8)], out.at[core], fsem.at[0], fsem.at[1])
    last.start()
    out[core] = done[pl.ds(8 * (1 - core), 8)]
    for j in range(2):
        for i in ALL:
            push(i, j).wait_send()

    @pl.when(core == 0)
    def _():
        for i in ALL:
            hand(i, 0).wait_send()
    y_there.wait_recv()
    last.wait_send()
    last.wait_recv()


def train_step(x, seed, weights):
    anywhere = pl.BlockSpec(memory_space=pl.ANY)
    vmem = pl.BlockSpec(memory_space=pltpu.VMEM)
    dma = pltpu.SemaphoreType.DMA
    act = lambda cols, dt=BF16: pltpu.VMEM((ROWS, cols), dt)
    saved = lambda cols, dt=BF16: jax.ShapeDtypeStruct((LAYERS - 1, ROWS, cols), dt)
    outs = pl.pallas_call(
        step_kernel,
        name="step",
        out_shape=[jax.ShapeDtypeStruct((2 * ROWS, D), BF16)] + [jax.ShapeDtypeStruct((2,) + s, BF16) for s in W_SHAPES]
        + [saved(D), saved(3 * D), saved(2 * D, F32), saved(D), saved(D), saved(QUAD * D), saved(QUAD * D)]
        + [jax.ShapeDtypeStruct((2, 8, NU) + TILE, F32)],
        in_specs=[anywhere] * 6,
        out_specs=[anywhere] * 12 + [vmem],
        scratch_shapes=[
            pltpu.VMEM((OWN_SLOTS + 4, NU) + CUBE + TILE, F32),
            pltpu.VMEM((4, NU) + CUBE + TILE, F32),
            pltpu.VMEM((CHUNKS, NU) + TILE, F32),
            act(D), act(3 * D), act(2 * D, F32), act(D), act(D), act(QUAD * D), act(QUAD * D), act(D), act(D), act(D),
        ] + [pltpu.VMEM(s, BF16) for s in W_SHAPES] + [
            dma((6,)), dma((7,)), dma, dma((6, 2)), dma((6, 2)), dma((2, 6)), dma((3,)), dma((QUAD,)), dma((QUAD,)), dma((2,)),
            pltpu.SemaphoreType.REGULAR((QUAD,)), pltpu.SemaphoreType.REGULAR((QUAD,)),
        ] + ring_scratch(),
        compiler_params=pltpu.CompilerParams(collective_id=1, has_side_effects=True, vmem_limit_bytes=67043328),
    )(x, seed, *weights)
    return outs[0], outs[-1]


def finish_kernel(y_in, sums, y, gq, go, gu, gd, buf, in_sem, out_sem):
    parts = buf.shape[0]
    move = lambda i, into: (pltpu.make_async_copy(y_in.at[i], buf.at[i], in_sem.at[i]) if into
                            else pltpu.make_async_copy(buf.at[i], y.at[i], out_sem.at[i]))
    for i in range(parts):
        move(i, True).start()
    outs = (gq, go, gu, gd)
    for layer in range(2):
        for tile in TILES:
            array, rg, col = tile
            q, half, unit = PLACE_OF[tile]
            outs[array][layer, rg * 8:rg * 8 + 8, col * LN:col * LN + LN] = sums[half, 4 * (1 - layer) + q, unit]
    for i in range(parts):
        move(i, True).wait()
        move(i, False).start()
    for i in range(parts):
        move(i, False).wait()


def finish(y, sums, parts=4):
    anywhere = pl.BlockSpec(memory_space=pl.ANY)
    vmem = pl.BlockSpec(memory_space=pltpu.VMEM)
    shape = (parts, 2 * ROWS // parts, D)
    return pl.pallas_call(
        finish_kernel,
        name="finish",
        out_shape=[jax.ShapeDtypeStruct(shape, BF16)]
        + [jax.ShapeDtypeStruct(s, F32) for s in ((2, 8, 3 * D), (2, 8, D), (2, 8, QUAD * D), (2, 32, D))],
        in_specs=[anywhere, vmem],
        out_specs=[anywhere] + [vmem] * 4,
        scratch_shapes=[pltpu.VMEM(shape, BF16), pltpu.SemaphoreType.DMA((parts,)), pltpu.SemaphoreType.DMA((parts,))],
    )(y.reshape(shape), sums)


def solution(mesh):
    def step(x_in, seed_grad, w_qkv, w_out, w_up, w_down):
        shape = x_in.shape
        weights = (w_qkv, w_out, w_up, w_down)
        y, sums = train_step(x_in.reshape(2 * ROWS, D), seed_grad.reshape(2 * ROWS, D), weights)
        y, *grads = finish(y, sums)
        return y.reshape(shape), *grads

    act, weight, grad = P(None, "dp"), P("pp"), P("pp", "dp")
    return jax.shard_map(
        step,
        mesh=mesh,
        in_specs=(act, act, weight, weight, weight, weight),
        out_specs=(act, grad, grad, grad, grad),
        check_vma=False,
    )
```

```python
import functools
import math

import jax
import jax.numpy as jnp
from jax import lax
from jax.experimental import pallas as pl
from jax.experimental.pallas import tpu as pltpu
from jax.sharding import PartitionSpec as P

F32 = jnp.float32
BF16 = jnp.bfloat16
MESH = pl.DeviceIdType.MESH

D = 512
HD = 64
LN = 128
TILE = (8, LN)
QUAD = 4
PLANE = (QUAD, QUAD)
CUBE = PLANE + (QUAD,)
NU = 6
SEQ = LN
NSEQ = 6
ROWS = NSEQ * SEQ
LAYERS = 4
EPS = 1e-6
GELU_C1 = math.sqrt(2.0 / math.pi)
GELU_C2 = GELU_C1 * 0.044715
EXP2_SCALE = HD ** -0.5 * math.log2(math.e)
W_SHAPES = ((D, 3 * D), (D, D), (D, QUAD * D), (QUAD * D, D))
LAST = (((1,), (1,)), ((), ()))
FIRST = (((0,), (0,)), ((), ()))


def dot(a, b):
    return jnp.dot(a, b, preferred_element_type=F32)


def dot_last(a, b):
    return lax.dot_general(a, b, LAST, preferred_element_type=F32)


def dot_first(a, b):
    return lax.dot_general(a, b, FIRST, preferred_element_type=F32)


def inv_rms(h):
    return lax.rsqrt(jnp.mean(h * h, axis=-1, keepdims=True) + EPS)


def rms_bwd(h, g):
    ir = inv_rms(h)
    n = h * ir
    return ir * (g - n * jnp.mean(g * n, axis=-1, keepdims=True))


def gelu(u):
    t = jnp.tanh(u * (GELU_C1 + GELU_C2 * (u * u)))
    return u * (0.5 * t + 0.5)


def gelu_slope(u):
    a = GELU_C2 * (u * u)
    t = jnp.tanh(u * (a + GELU_C1))
    half = 0.5 * t + 0.5
    return half + u * half * (1.0 - t) * (3.0 * a + GELU_C1)


def block_diag(x):
    first = lax.broadcasted_iota(jnp.int32, (SEQ, 2 * HD), 1) < HD
    zero = jnp.zeros_like(x)
    return jnp.concatenate([jnp.where(first, x, zero), jnp.where(first, zero, x)], axis=0)


def units_of(step, n_seqs):
    return [(pl.ds(pl.multiple_of((step * n_seqs + n) * SEQ, SEQ), SEQ), pair) for n in range(n_seqs) for pair in range(QUAD)]


def attention_fwd(step, n_seqs, qkv, p_out, o_out):
    key = lax.broadcasted_iota(jnp.int32, (SEQ, SEQ), 0)
    query = lax.broadcasted_iota(jnp.int32, (SEQ, SEQ), 1)
    allowed = key <= query
    units = units_of(step, n_seqs)

    def scores(rows, pair):
        c = pair * LN
        return dot_last(qkv[rows, D + c:D + c + LN], block_diag(qkv[rows, c:c + LN]))

    ahead = 2
    pending = [scores(*u) for u in units[:ahead]]
    for i, (rows, pair) in enumerate(units):
        if i + ahead < len(units):
            pending.append(scores(*units[i + ahead]))
        s = pending[i]
        c = pair * LN
        probs = []
        for head in range(2):
            sh = jnp.where(allowed, s[:, head * LN:head * LN + LN], -1e30)
            e = jnp.exp2((sh - jnp.max(sh, axis=0, keepdims=True)) * EXP2_SCALE)
            p = e * (1.0 / jnp.sum(e, axis=0, keepdims=True))
            p_out[rows, 2 * c + head * LN:2 * c + head * LN + LN] = p
            probs.append(p.astype(BF16))
        v = qkv[rows, 2 * D + c:2 * D + c + LN]
        o_out[rows, c:c + LN] = dot_first(jnp.concatenate(probs, axis=0), block_diag(v)).astype(BF16)


def attention_bwd(step, n_seqs, qkv, p_in, do):
    units = units_of(step, n_seqs)

    def first(rows, pair):
        c = pair * LN
        d = block_diag(do[rows, c:c + LN])
        return d, dot_last(qkv[rows, 2 * D + c:2 * D + c + LN], d)

    ahead = 2
    pending = [first(*u) for u in units[:ahead]]
    for i, (rows, pair) in enumerate(units):
        if i + ahead < len(units):
            pending.append(first(*units[i + ahead]))
        d, dp = pending[i]
        c = pair * LN
        q = qkv[rows, c:c + LN]
        k = qkv[rows, D + c:D + c + LN]
        p = p_in[rows, 2 * c:2 * c + 256]
        dv = dot(p.astype(BF16), d).astype(BF16)
        pd = p * dp
        ds = ((pd - p * jnp.sum(pd, axis=0, keepdims=True)) * HD ** -0.5).astype(BF16)
        dk = dot(ds, block_diag(q)).astype(BF16)
        dq = dot_first(jnp.concatenate([ds[:, :LN], ds[:, LN:]], axis=0), block_diag(k)).astype(BF16)
        qkv[rows, c:c + LN] = dq
        qkv[rows, D + c:D + c + LN] = dk
        qkv[rows, 2 * D + c:2 * D + c + LN] = dv


AXES = (("x", "y", "z"), ("y", "z", "x"), ("z", "x", "y"))
NAT = ("z", "y", "x")
STRIDE = {"x": 1, "y": 4, "z": 16}
UNITS = [(colour, way) for colour in range(3) for way in (1, -1)]


class Place:
    def __init__(self):
        self.core = lax.axis_index("pp")
        self.dp = lax.axis_index("dp")
        self.at = {"x": lax.rem(self.dp, QUAD), "y": lax.rem(self.dp // QUAD, QUAD), "z": self.dp // 16}

    def neighbour(self, axis, way):
        c = self.at[axis]
        return (self.core, self.dp + (lax.rem(c + way + QUAD, QUAD) - c) * STRIDE[axis])

    def partner(self):
        return (1 - self.core, self.dp)

    def block(self, axis, way, step):
        return lax.rem(self.at[axis] - way * (1 + step) + 8, QUAD)


def greet(peers):
    barrier = pltpu.get_barrier_semaphore()
    for p in peers:
        pl.semaphore_signal(barrier, inc=1, device_id=p, device_id_type=MESH)
    pl.semaphore_wait(barrier, len(peers))


CHUNKS = 16
PERIOD = 3
STREAMS = 4
SLOTS = PERIOD * CHUNKS
HOP = (16, 4, 1)
FROM = (0, 16, 20)
LINK = 21


def ring_scratch():
    dma = pltpu.SemaphoreType.DMA
    return [
        pltpu.VMEM((STREAMS, NU, LINK) + TILE, F32), pltpu.VMEM((STREAMS, 2, NU, LINK) + TILE, F32),
        pltpu.VMEM((STREAMS, NU) + PLANE + TILE, F32), pltpu.VMEM((STREAMS, NU, 4) + TILE, F32),
        pltpu.VMEM((STREAMS, 3, NU, 4) + TILE, F32), pltpu.VMEM((2, STREAMS, 3, NU) + TILE, F32),
        dma((STREAMS,)), dma((STREAMS, 2)), dma((3, STREAMS)), dma((3, STREAMS)),
    ]


def pick_block(ref, axis, b):
    return {"z": lambda: ref[b], "y": lambda: ref[:, b], "x": lambda: ref[:, :, b]}[axis]()


class Rings:
    def __init__(self, place, scratch, own, ready, done):
        self.p, self.own, self.ready, self.done = place, own, ready, done
        self.sent, self.got, self.t1, self.t2, self.d2, self.d3, self.ss, self.rs, self.ds, self.dr = scratch
        self.sent[:, :, FROM[1]:] = jnp.zeros((STREAMS, NU, LINK - FROM[1]) + TILE, F32)

    def links(self, e, par, link, lo):
        tiles = pl.ds(lo, LINK - lo)
        axis, way = UNITS[0 if link is None else link]
        at = slice(None) if link is None else link
        return pltpu.make_async_remote_copy(self.sent.at[e, at, tiles], self.got.at[e, par, at, tiles], self.ss.at[e], self.rs.at[e, par],
                                            device_id=self.p.neighbour("xyz"[axis], way), device_id_type=MESH)

    def wait(self, e, par, lo):
        c = self.links(e, par, None, lo)
        c.wait_send()
        c.wait_recv()

    def send(self, e, par, lo):
        for link in range(NU):
            self.links(e, par, link, lo).start()

    def link(self, u, phase):
        return (u + 2 * phase) % NU

    def came(self, e, par, u, phase):
        lo = FROM[phase]
        v = self.got[e, par, self.link(u, phase), lo:lo + HOP[phase]]
        return v.reshape((PLANE, PLANE[1:], ())[phase] + TILE)

    def go(self, e, u, phase, value):
        lo = FROM[phase]
        self.sent[e, self.link(u, phase), lo:lo + HOP[phase]] = value.reshape((HOP[phase],) + TILE)

    def block(self, u, phase, step):
        colour, way = UNITS[u]
        return self.p.block(AXES[colour][phase], way, step)

    def first(self, own, u, step):
        return pick_block(own.at[u], AXES[UNITS[u][0]][0], self.block(u, 0, step))

    def second_ref(self, e, u, b):
        order = AXES[UNITS[u][0]]
        rest = [a for a in NAT if a != order[0]]
        return self.t1.at[(e, u, slice(None), b) if rest.index(order[1]) == 1 else (e, u, b)]

    def second(self, e, u, step):
        return self.second_ref(e, u, self.block(u, 1, step))[...]

    def third(self, e, u, step):
        return self.t2[e, u, self.block(u, 2, step)]

    def straight(self, e, kind, u, j):
        phase = 1 if kind == 0 else 2
        axis = AXES[UNITS[u][0]][phase]
        b = lax.rem(self.p.at[axis] + j, QUAD)
        src = self.second_ref(e, u, b) if kind == 0 else self.t2.at[e, u, b]
        dst = self.landing(e, kind).at[j - 1, u]
        return pltpu.make_async_remote_copy(src, dst, self.ds.at[kind, e], self.dr.at[kind, e],
                                            device_id=self.p.neighbour(axis, j), device_id_type=MESH)

    def landing(self, e, kind):
        return self.d2.at[e] if kind == 0 else self.d3.at[kind - 1, e]

    def go_straight(self, e, kind):
        for j in (1, 3, 2):
            for u in range(NU):
                self.straight(e, kind, u, j).start()

    def wait_straight(self, e, kind):
        at = self.landing(e, kind)
        c = pltpu.make_async_remote_copy(at, at, self.ds.at[kind, e], self.dr.at[kind, e],
                                         device_id=self.p.neighbour("x", 1), device_id_type=MESH)
        c.wait_send()
        c.wait_recv()

    def sum_straight(self, e, kind, u):
        at = self.landing(e, kind)
        return at[0, u] + at[1, u] + at[2, u]

    def slot(self, s, step, drain=False):
        e = lax.rem(s, STREAMS)
        par = lax.rem(s // STREAMS, 2)
        old = 1 - par
        since = s - STREAMS * step
        chunk = lambda i: since // PERIOD - STREAMS * i
        live = lambda i: (since >= PERIOD * STREAMS * i) & (chunk(i) < CHUNKS)
        early = lambda i: chunk(i) < CHUNKS - 2 * STREAMS
        not_late = lambda i: chunk(i) < CHUNKS - STREAMS
        if not drain:
            early = not_late = lambda i: True
        both = lambda a, b: a if b is True else a & b
        ring1 = both(live(1), not_late(1))
        ring2 = both(live(2), early(2))
        late = live(1) & jnp.logical_not(not_late(1)) if drain else None
        middle = live(2) & not_late(2) & jnp.logical_not(early(2)) if drain else None
        if step == 0:
            was, more = live(1), both(live(2), not_late(2)) | both(live(3), early(3))
        else:
            was, more = live(0), ring1 | ring2

        @pl.when(was)
        def _():
            self.wait(e, old, 0)

        @pl.when(jnp.logical_not(was) & more)
        def _():
            self.wait(e, old, FROM[1])

        if step == 0:
            @pl.when(both(live(3), early(3)))
            def _():
                for u in range(NU):
                    self.done[chunk(3), u] = self.came(e, old, u, 2) + self.third(e, u, 3)

            @pl.when(both(live(2), not_late(2)))
            def _():
                for u in range(NU):
                    self.t2[e, u] = self.came(e, old, u, 1) + self.second(e, u, 3)
                    self.go(e, u, 2, self.third(e, u, 0))

            @pl.when(live(1))
            def _():
                own = self.own(chunk(1))
                for u in range(NU):
                    self.t1[e, u] = self.came(e, old, u, 0) + self.first(own, u, 3)
                    self.go(e, u, 1, self.second(e, u, 0))

            @pl.when(live(0))
            def _():
                self.ready(chunk(0))
                own = self.own(chunk(0))
                for u in range(NU):
                    self.go(e, u, 0, self.first(own, u, 0))
        else:
            @pl.when(ring2)
            def _():
                for u in range(NU):
                    self.go(e, u, 2, self.came(e, old, u, 2) + self.third(e, u, step))

            if drain and step == 1:
                @pl.when(middle)
                def _():
                    self.wait_straight(e, 2)
                    for u in range(NU):
                        self.done[chunk(2), u] = self.sum_straight(e, 2, u) + self.third(e, u, 3)

            @pl.when(ring1)
            def _():
                for u in range(NU):
                    self.go(e, u, 1, self.came(e, old, u, 1) + self.second(e, u, step))

            if drain:
                @pl.when(late)
                def _():
                    self.wait_straight(e, step - 1)
                    for u in range(NU):
                        if step == 1:
                            self.t2[e, u] = self.sum_straight(e, 0, u) + self.second(e, u, 3)
                        else:
                            self.done[chunk(1), u] = self.sum_straight(e, 1, u) + self.third(e, u, 3)

            @pl.when(live(0))
            def _():
                own = self.own(chunk(0))
                for u in range(NU):
                    self.go(e, u, 0, self.came(e, old, u, 0) + self.first(own, u, step))

        @pl.when(live(0))
        def _():
            self.send(e, par, 0)

        @pl.when(jnp.logical_not(live(0)) & (ring1 | ring2))
        def _():
            self.send(e, par, FROM[1])

        if drain and step < 2:
            @pl.when(late)
            def _():
                self.go_straight(e, step)

        if drain and step == 0:
            @pl.when(middle)
            def _():
                self.go_straight(e, 2)

    def step_of(self, s):
        return s * (STREAMS % PERIOD) % PERIOD if isinstance(s, int) else lax.rem(s * (STREAMS % PERIOD), PERIOD)

    def drain(self, start):
        def one(s, _):
            at = self.step_of(s)
            for step in range(PERIOD):
                @pl.when(at == step)
                def _():
                    self.slot(s, step, True)
            return 0

        lax.fori_loop(start, SLOTS - PERIOD + 5 * STREAMS + 1, one, 0)


def tiles_of_layer():
    down = [(3, g, j) for j in range(QUAD) for g in range(QUAD)]
    up = [(2, 0, j) for j in range(16)]
    out = [(1, 0, j) for j in range(QUAD)]
    qkv = [(0, 0, j) for j in range(12)]
    return down + up + out + qkv


TILES = tiles_of_layer()
PLACE_OF = {t: (i // 12, i % 12 // 6, i % 6) for i, t in enumerate(TILES)}


FWD_SEQS = 6
BWD_SEQS = 3
OWN_SLOTS = 7
SENT_SLOTS = 3
LEAD = 3
QKV_W, OUT_W, UP_W, DOWN_W = range(4)
HALF = 2 * D
PIECES = [(QKV_W, ()), (OUT_W, ()), (UP_W, (slice(None), pl.ds(0, HALF))), (DOWN_W, (pl.ds(0, HALF),)),
          (UP_W, (slice(None), pl.ds(HALF, HALF))), (DOWN_W, (pl.ds(HALF, HALF),))]
ALL = range(len(PIECES))
QKV_P, OUT_P, UP_P, DOWN_P = (0,), (1,), (2, 4), (3, 5)


def step_kernel(x, seed, wq, wo, wu, wd,
                y, rq, ro, ru, rd, hs, qs, ps, os, ms, us, es, out,
                grads, recv, done, h, qkv, p, o, m, u, e, g, g1, do, vq, vo, vu, vd,
                wsem, asem, gsem, psem, qsem, hsem, ysem, dsend, drecv, fsem, credit, wfree, *ring):
    place = Place()
    core = place.core
    partner = place.partner()
    mine = (wq, wo, wu, wd)
    theirs = (rq, ro, ru, rd)
    held = (vq, vo, vu, vd)
    acts = ((h, hs), (qkv, qs), (p, ps), (o, os), (m, ms), (u, us), (e, es))
    H, QKV, PROB, O, M, U, E = range(7)
    rows = pl.ds(core * ROWS, ROWS)

    def to_partner(src, dst, send, arrive):
        return pltpu.make_async_remote_copy(src, dst, send, arrive, device_id=partner, device_id_type=MESH)

    def piece_of(ref, i):
        at = PIECES[i][1]
        return ref.at[at] if at else ref

    def push(i, j):
        k = PIECES[i][0]
        return to_partner(piece_of(mine[k].at[j], i), piece_of(theirs[k].at[j], i), psem.at[i, j], qsem.at[i, j])

    def hand(i, l):
        k = PIECES[i][0]
        return to_partner(piece_of(mine[k].at[l], i), piece_of(held[k], i), hsem.at[0, i], hsem.at[1, i])

    def local_w(i, l, src):
        k = PIECES[i][0]
        return pltpu.make_async_copy(piece_of(src[k].at[lax.rem(l, 2)], i), piece_of(held[k], i), wsem.at[i])

    def fetch_w(i, l, arrives):
        @pl.when(l // 2 == core)
        def _():
            local_w(i, l, mine).start()

        @pl.when(l // 2 != core)
        def _():
            @pl.when(arrives)
            def _():
                push(i, lax.rem(l, 2)).wait_recv()
            local_w(i, l, theirs).start()

    def wait_w(*pieces):
        for i in pieces:
            local_w(i, 0, mine).wait()

    def act(i, l, back):
        vmem, hbm = acts[i]
        return pltpu.make_async_copy(hbm.at[l], vmem, asem.at[i]) if back else pltpu.make_async_copy(vmem, hbm.at[l], asem.at[i])

    def own_slot(chunk):
        return lax.rem(chunk, OWN_SLOTS)

    def sent_slot(chunk):
        return lax.rem(chunk, SENT_SLOTS)

    def cross(chunk):
        q = sent_slot(chunk)
        return to_partner(grads.at[OWN_SLOTS + q], recv.at[q], dsend.at[q], drecv.at[q])

    def ready(chunk):
        q = sent_slot(chunk)
        cross(chunk).wait_recv()
        for unit in range(NU):
            grads[own_slot(chunk), unit] = grads[own_slot(chunk), unit] + recv[q, unit]

        @pl.when(chunk + SENT_SLOTS < CHUNKS)
        def _():
            pl.semaphore_signal(credit.at[q], inc=1, device_id=partner, device_id_type=MESH)

    rings = Rings(place, ring, lambda chunk: grads.at[own_slot(chunk)], ready, done)

    x_in = pltpu.make_async_copy(x.at[rows], h, asem.at[H])
    x_in.start()
    seed_in = pltpu.make_async_copy(seed.at[rows], g, gsem)

    @pl.when(core == 0)
    def _():
        for i in ALL:
            local_w(i, 0, mine).start()
    greet([partner] + [place.neighbour(a, way) for a in NAT for way in (1, -1, 2)])

    @pl.when(core == 0)
    def _():
        for i in ALL:
            hand(i, 0).start()

    @pl.when(core == 1)
    def _():
        for j in range(2):
            for i in ALL:
                push(i, j).start()
    seed_in.start()
    x_in.wait()

    def layer(l, _):
        handed = (l < 2) & (core == 1)

        def weight(*pieces):
            @pl.when(jnp.logical_not(handed))
            def _():
                wait_w(*pieces)

            @pl.when(handed)
            def _():
                for i in pieces:
                    hand(i, 0).wait_recv()

        def used(group):
            @pl.when((l == 0) & (core == 1))
            def _():
                pl.semaphore_signal(wfree.at[group], inc=1, device_id=partner, device_id_type=MESH)

        def hand_on(at, group, *pieces):
            @pl.when((l == at) & (core == 0))
            def _():
                pl.semaphore_wait(wfree.at[group], 1)
                for i in pieces:
                    hand(i, 0).wait_send()
                    hand(i, 1).start()

        def again(i):
            @pl.when(l > 0)
            def _():
                act(i, l - 1, False).wait()

        def save(i):
            @pl.when(l < LAYERS - 1)
            def _():
                act(i, l, False).start()

        def next_w(when, to, *pieces):
            @pl.when(when)
            def _():
                for i in pieces:
                    fetch_w(i, to, True)

        more = l < LAYERS - 1
        again(H)

        @pl.when(l > 0)
        def _():
            h[...] = do[...]
        save(H)
        weight(0)
        again(QKV)
        hf = h[...].astype(F32)
        qkv[...] = dot((hf * inv_rms(hf)).astype(BF16), vq[...]).astype(BF16)
        used(0)
        save(QKV)
        again(PROB)
        again(O)

        for i in range(NSEQ // FWD_SEQS):
            attention_fwd(i, FWD_SEQS, qkv, p, o)
        hand_on(0, 0, 0)
        hand_on(1, 3, 4, 5)
        save(PROB)
        save(O)
        weight(1)
        again(M)
        mb = (h[...].astype(F32) + dot(o[...], vo[...])).astype(BF16)
        m[...] = mb
        mf = mb.astype(F32)
        g1[...] = (mf * inv_rms(mf)).astype(BF16)
        used(1)
        save(M)
        again(U)
        again(E)
        weight(2, 3)

        def mlp(j):
            cols = slice(j * HALF, (j + 1) * HALF)
            ub = dot(g1[...], vu[:, cols]).astype(BF16)
            u[:, cols] = ub
            eb = gelu(ub.astype(F32)).astype(BF16)
            e[:, cols] = eb
            return dot(eb, vd[cols, :])

        half_way = m[...].astype(F32) + mlp(0)
        for unit in range(NU):
            for col in range(QUAD):
                grads[0, unit, :, :, col] = half_way[unit * SEQ:unit * SEQ + SEQ, col * LN:col * LN + LN].reshape(PLANE + TILE)
        used(2)
        hand_on(0, 1, 1)
        mine_next = more & jnp.logical_or(l > 0, core == 0)
        next_w(mine_next, l + 1, 0, 1)
        weight(4, 5)
        rest = mlp(1)
        for unit in range(NU):
            part = pl.ds(unit * SEQ, SEQ)
            for col in range(QUAD):
                cols = slice(col * LN, col * LN + LN)
                do[part, cols] = (grads[0, unit, :, :, col].reshape((SEQ, LN)) + rest[unit * SEQ:unit * SEQ + SEQ, cols]).astype(BF16)
        used(3)
        hand_on(0, 2, 2, 3)
        next_w(mine_next, l + 1, 2, 3, 4, 5)

        @pl.when((l == 1) & (core == 0))
        def _():
            for j in (1, 0):
                for i in ALL:
                    push(i, j).start()
        save(U)
        save(E)
        return 0

    lax.fori_loop(0, LAYERS, layer, 0)
    y_here = pltpu.make_async_copy(do, y.at[rows], ysem.at[0])
    y_there = to_partner(do, y.at[rows], ysem.at[1], ysem.at[2])
    y_here.start()
    y_there.start()

    def free(chunk):
        @pl.when(chunk >= SENT_SLOTS)
        def _():
            cross(chunk).wait_send()

    def put(base, tile, value):
        q, half, unit = PLACE_OF[tile]
        index = jnp.where(core == half, own_slot(base + q), OWN_SLOTS + sent_slot(base + q))
        grads[index, unit] = value.reshape(CUBE + TILE)

    def ship(chunk):
        @pl.when(chunk >= SENT_SLOTS)
        def _():
            pl.semaphore_wait(credit.at[sent_slot(chunk)], 1)
        cross(chunk).start()

    def down_grad(base, halves):
        for half in halves:
            if half == 0:
                free(base)
                free(base + 1)
            w = dot_first(e[...], g[:, half * 256:half * 256 + 256]).reshape((64, QUAD, 8, 256))
            for j in range(2):
                for rg in range(QUAD):
                    put(base, (DOWN_W, rg, 2 * half + j), w[:, rg, :, j * LN:j * LN + LN])
            if half == 1:
                ship(base)

    def gelu_part(lo, hi):
        de = dot_last(g[...], vd[lo:hi, :])
        u[:, lo:hi] = (gelu_slope(u[:, lo:hi].astype(F32)) * de).astype(BF16)

    def wide_grad(base, array, a, b, parts):
        for part in parts:
            w = dot_first(a, b[:, part * D:part * D + D]).reshape((64, 8, D))
            for j in range(QUAD):
                put(base, (array, 0, QUAD * part + j), w[:, :, j * LN:j * LN + LN])

    seed_in.wait()
    down_grad(0, range(2))
    act(E, LAYERS - 2, True).start()
    y_here.wait()
    y_there.wait_send()

    def iteration(it, _):
        l = LAYERS - 1 - it
        more = it < LAYERS - 1
        base = 4 * it

        def loaded(acts_of, pieces=()):
            @pl.when(it > 0)
            def _():
                for i in acts_of:
                    act(i, l, True).wait()
                wait_w(*pieces)

        def after(acts_of, pieces=()):
            @pl.when(more)
            def _():
                for i in pieces:
                    fetch_w(i, l - 1, l <= 2)
                for i in acts_of:
                    act(i, l - 1, True).start()

        def piece(n):
            if n == 0:
                loaded((U,), DOWN_P)
                gelu_part(0, 3 * 256)
            elif n == 1:
                gelu_part(3 * 256, 3 * D)
            elif n == 2:
                gelu_part(3 * D, QUAD * D)
                after((), DOWN_P)
                loaded((M,))
                mf = m[...].astype(F32)
                g1[...] = (mf * inv_rms(mf)).astype(BF16)
                wide_grad(base, UP_W, g1[...], u, (0,))
            elif n == 3:
                free(base + 2)
                wide_grad(base, UP_W, g1[...], u, (1, 2, 3))
                ship(base + 1)
            elif n == 4:
                loaded((), UP_P)
                dc = dot_last(u[...], vu[...])
                g1[...] = (g[...].astype(F32) + rms_bwd(m[...].astype(F32), dc)).astype(BF16)
                after((U, M), UP_P)
            elif n == 5:
                loaded((O,), OUT_P)
                do[...] = dot_last(g1[...], vo[...]).astype(BF16)
                wide_grad(base, OUT_W, o[...], g1, (0,))
                ship(base + 2)
                after((O,), OUT_P)
            elif n in (6, 7):
                if n == 6:
                    loaded((PROB, QKV))
                attention_bwd(n - 6, BWD_SEQS, qkv, p, do)
                if n == 7:
                    after((PROB,))
            elif n == 8:
                loaded((H,))
                free(base + 3)
                hf = h[...].astype(F32)
                wide_grad(base, QKV_W, (hf * inv_rms(hf)).astype(BF16), qkv, range(3))
                ship(base + 3)
            elif n == 9:
                loaded((), QKV_P)
                da = dot_last(qkv[...], vq[...])
                g[...] = (g1[...].astype(F32) + rms_bwd(h[...].astype(F32), da)).astype(BF16)
                after((H, QKV), QKV_P)
            else:
                @pl.when(more)
                def _():
                    if n == 10:
                        act(E, l - 1, True).wait()
                    down_grad(base + QUAD, (n - 10,))

                if n == 11:
                    @pl.when(l > 1)
                    def _():
                        act(E, l - 2, True).start()

        for n in range(12):
            s = 12 * it + n - LEAD
            step = rings.step_of(n + 2 * PERIOD - LEAD)
            if n < LEAD:
                @pl.when(it > 0)
                def _():
                    rings.slot(s, step)
            else:
                rings.slot(s, step)
            piece(n)
        return 0

    lax.fori_loop(0, LAYERS, iteration, 0)
    rings.drain(SLOTS - LEAD)

    for q in range(SENT_SLOTS):
        cross(q).wait_send()
    last = to_partner(done.at[pl.ds(8 * core, 8)], out.at[core], fsem.at[0], fsem.at[1])
    last.start()
    kept = pltpu.make_async_copy(done.at[pl.ds(8 * (1 - core), 8)], out.at[core], gsem)
    kept.start()
    for j in range(2):
        for i in ALL:
            push(i, j).wait_send()

    @pl.when(core == 0)
    def _():
        for i in ALL:
            hand(i, 0).wait_send()
    y_there.wait_recv()
    kept.wait()
    last.wait_send()
    last.wait_recv()


def train_step(x, seed, weights):
    anywhere = pl.BlockSpec(memory_space=pl.ANY)
    dma = pltpu.SemaphoreType.DMA
    act = lambda cols, dt=BF16: pltpu.VMEM((ROWS, cols), dt)
    saved = lambda cols, dt=BF16: jax.ShapeDtypeStruct((LAYERS - 1, ROWS, cols), dt)
    outs = pl.pallas_call(
        step_kernel,
        name="step",
        out_shape=[jax.ShapeDtypeStruct((2 * ROWS, D), BF16)] + [jax.ShapeDtypeStruct((2,) + s, BF16) for s in W_SHAPES]
        + [saved(D), saved(3 * D), saved(2 * D, F32), saved(D), saved(D), saved(QUAD * D), saved(QUAD * D)]
        + [jax.ShapeDtypeStruct((2, 8, NU) + TILE, F32)],
        in_specs=[anywhere] * 6,
        out_specs=[anywhere] * 13,
        scratch_shapes=[
            pltpu.VMEM((OWN_SLOTS + SENT_SLOTS, NU) + CUBE + TILE, F32),
            pltpu.VMEM((SENT_SLOTS, NU) + CUBE + TILE, F32),
            pltpu.VMEM((CHUNKS, NU) + TILE, F32),
            act(D), act(3 * D), act(2 * D, F32), act(D), act(D), act(QUAD * D), act(QUAD * D), act(D), act(D), act(D),
        ] + [pltpu.VMEM(s, BF16) for s in W_SHAPES] + [
            dma((6,)), dma((7,)), dma, dma((6, 2)), dma((6, 2)), dma((2, 6)), dma((3,)), dma((QUAD,)), dma((QUAD,)), dma((2,)),
            pltpu.SemaphoreType.REGULAR((QUAD,)), pltpu.SemaphoreType.REGULAR((QUAD,)),
        ] + ring_scratch(),
        compiler_params=pltpu.CompilerParams(collective_id=1, has_side_effects=True, vmem_limit_bytes=67043328),
    )(x, seed, *weights)
    return outs[0], outs[-1]


def finish_kernel(y_in, sums_in, y, gq, go, gu, gd, buf, sums, in_sem, out_sem, sum_sem):
    parts = buf.shape[0]
    here = pltpu.make_async_copy(sums_in, sums, sum_sem)
    here.start()
    into = [pltpu.make_async_copy(y_in.at[i], buf.at[i], in_sem.at[i]) for i in range(parts)]
    out = [pltpu.make_async_copy(buf.at[i], y.at[i], out_sem.at[i]) for i in range(parts)]
    for c in into:
        c.start()
    here.wait()
    outs = (gq, go, gu, gd)
    for layer in range(2):
        for tile in TILES:
            array, rg, col = tile
            q, half, unit = PLACE_OF[tile]
            outs[array][layer, rg * 8:rg * 8 + 8, col * LN:col * LN + LN] = sums[half, QUAD * (1 - layer) + q, unit]
    for c, d in zip(into, out):
        c.wait()
        d.start()
    for d in out:
        d.wait()


def finish(y, sums, parts=6):
    anywhere = pl.BlockSpec(memory_space=pl.ANY)
    vmem = pl.BlockSpec(memory_space=pltpu.VMEM)
    dma = pltpu.SemaphoreType.DMA
    shape = (parts, 2 * ROWS // parts, D)
    return pl.pallas_call(
        finish_kernel,
        name="finish",
        out_shape=[jax.ShapeDtypeStruct(shape, BF16)]
        + [jax.ShapeDtypeStruct(s, F32) for s in ((2, 8, 3 * D), (2, 8, D), (2, 8, QUAD * D), (2, 32, D))],
        in_specs=[anywhere] * 2,
        out_specs=[anywhere] + [vmem] * QUAD,
        scratch_shapes=[pltpu.VMEM(shape, BF16), pltpu.VMEM(sums.shape, F32), dma((parts,)), dma((parts,)), dma],
    )(y.reshape(shape), sums)


def solution(mesh):
    def step(x_in, seed_grad, w_qkv, w_out, w_up, w_down):
        shape = x_in.shape
        weights = (w_qkv, w_out, w_up, w_down)
        y, sums = train_step(x_in.reshape(2 * ROWS, D), seed_grad.reshape(2 * ROWS, D), weights)
        y, *grads = finish(y, sums)
        return y.reshape(shape), *grads

    act, weight, grad = P(None, "dp"), P("pp"), P("pp", "dp")
    return jax.shard_map(
        step,
        mesh=mesh,
        in_specs=(act, act, weight, weight, weight, weight),
        out_specs=(act, grad, grad, grad, grad),
        check_vma=False,
    )
```

```python
import functools
import math

import jax
import jax.numpy as jnp
from jax import lax
from jax.experimental import pallas as pl
from jax.experimental.pallas import tpu as pltpu
from jax.sharding import PartitionSpec as P

F32 = jnp.float32
BF16 = jnp.bfloat16
MESH = pl.DeviceIdType.MESH

D = 512
HD = 64
LN = 128
TILE = (8, LN)
QUAD = 4
PLANE = (QUAD, QUAD)
CUBE = PLANE + (QUAD,)
NU = 6
SEQ = LN
NSEQ = 6
ROWS = NSEQ * SEQ
LAYERS = 4
EPS = 1e-6
GELU_C1 = math.sqrt(2.0 / math.pi)
GELU_C2 = GELU_C1 * 0.044715
EXP2_SCALE = HD ** -0.5 * math.log2(math.e)
W_SHAPES = ((D, 3 * D), (D, D), (D, QUAD * D), (QUAD * D, D))
LAST = (((1,), (1,)), ((), ()))
FIRST = (((0,), (0,)), ((), ()))


def dot(a, b):
    return jnp.dot(a, b, preferred_element_type=F32)


def dot_last(a, b):
    return lax.dot_general(a, b, LAST, preferred_element_type=F32)


def dot_first(a, b):
    return lax.dot_general(a, b, FIRST, preferred_element_type=F32)


def inv_rms(h):
    return lax.rsqrt(jnp.mean(h * h, axis=-1, keepdims=True) + EPS)


def rms_bwd(h, g):
    ir = inv_rms(h)
    n = h * ir
    return ir * (g - n * jnp.mean(g * n, axis=-1, keepdims=True))


def gelu(u):
    t = jnp.tanh(u * (GELU_C1 + GELU_C2 * (u * u)))
    return u * (0.5 * t + 0.5)


def gelu_slope(u):
    a = GELU_C2 * (u * u)
    t = jnp.tanh(u * (a + GELU_C1))
    half = 0.5 * t + 0.5
    return half + u * half * (1.0 - t) * (3.0 * a + GELU_C1)


def block_diag(x):
    first = lax.broadcasted_iota(jnp.int32, (SEQ, 2 * HD), 1) < HD
    zero = jnp.zeros_like(x)
    return jnp.concatenate([jnp.where(first, x, zero), jnp.where(first, zero, x)], axis=0)


def units_of(step, n_seqs):
    return [(pl.ds(pl.multiple_of((step * n_seqs + n) * SEQ, SEQ), SEQ), pair) for n in range(n_seqs) for pair in range(QUAD)]


def attention_fwd(step, n_seqs, qkv, p_out, o_out):
    key = lax.broadcasted_iota(jnp.int32, (SEQ, SEQ), 0)
    query = lax.broadcasted_iota(jnp.int32, (SEQ, SEQ), 1)
    allowed = key <= query
    units = units_of(step, n_seqs)

    def scores(rows, pair):
        c = pair * LN
        return dot_last(qkv[rows, D + c:D + c + LN], block_diag(qkv[rows, c:c + LN]))

    ahead = 2
    pending = [scores(*u) for u in units[:ahead]]
    for i, (rows, pair) in enumerate(units):
        if i + ahead < len(units):
            pending.append(scores(*units[i + ahead]))
        s = pending[i]
        c = pair * LN
        probs = []
        for head in range(2):
            sh = jnp.where(allowed, s[:, head * LN:head * LN + LN], -1e30)
            e = jnp.exp2((sh - jnp.max(sh, axis=0, keepdims=True)) * EXP2_SCALE)
            p = e * (1.0 / jnp.sum(e, axis=0, keepdims=True))
            p_out[rows, 2 * c + head * LN:2 * c + head * LN + LN] = p
            probs.append(p.astype(BF16))
        v = qkv[rows, 2 * D + c:2 * D + c + LN]
        o_out[rows, c:c + LN] = dot_first(jnp.concatenate(probs, axis=0), block_diag(v)).astype(BF16)


def attention_bwd(step, n_seqs, qkv, p_in, do):
    units = units_of(step, n_seqs)

    def first(rows, pair):
        c = pair * LN
        d = block_diag(do[rows, c:c + LN])
        return d, dot_last(qkv[rows, 2 * D + c:2 * D + c + LN], d)

    ahead = 2
    pending = [first(*u) for u in units[:ahead]]
    for i, (rows, pair) in enumerate(units):
        if i + ahead < len(units):
            pending.append(first(*units[i + ahead]))
        d, dp = pending[i]
        c = pair * LN
        q = qkv[rows, c:c + LN]
        k = qkv[rows, D + c:D + c + LN]
        p = p_in[rows, 2 * c:2 * c + 256]
        dv = dot(p.astype(BF16), d).astype(BF16)
        pd = p * dp
        ds = ((pd - p * jnp.sum(pd, axis=0, keepdims=True)) * HD ** -0.5).astype(BF16)
        dk = dot(ds, block_diag(q)).astype(BF16)
        dq = dot_first(jnp.concatenate([ds[:, :LN], ds[:, LN:]], axis=0), block_diag(k)).astype(BF16)
        qkv[rows, c:c + LN] = dq
        qkv[rows, D + c:D + c + LN] = dk
        qkv[rows, 2 * D + c:2 * D + c + LN] = dv


AXES = (("x", "y", "z"), ("y", "z", "x"), ("z", "x", "y"))
NAT = ("z", "y", "x")
STRIDE = {"x": 1, "y": 4, "z": 16}
UNITS = [(colour, way) for colour in range(3) for way in (1, -1)]


class Place:
    def __init__(self):
        self.core = lax.axis_index("pp")
        self.dp = lax.axis_index("dp")
        self.at = {"x": lax.rem(self.dp, QUAD), "y": lax.rem(self.dp // QUAD, QUAD), "z": self.dp // 16}

    def neighbour(self, axis, way):
        c = self.at[axis]
        return (self.core, self.dp + (lax.rem(c + way + QUAD, QUAD) - c) * STRIDE[axis])

    def partner(self):
        return (1 - self.core, self.dp)

    def block(self, axis, way, step):
        return lax.rem(self.at[axis] - way * (1 + step) + 8, QUAD)


def greet(peers):
    barrier = pltpu.get_barrier_semaphore()
    for p in peers:
        pl.semaphore_signal(barrier, inc=1, device_id=p, device_id_type=MESH)
    pl.semaphore_wait(barrier, len(peers))


CHUNKS = 16
PERIOD = 3
STREAMS = 4
SLOTS = PERIOD * CHUNKS
HOP = (16, 4, 1)
FROM = (0, 16, 20)
LINK = 21


def ring_scratch():
    dma = pltpu.SemaphoreType.DMA
    return [
        pltpu.VMEM((STREAMS, NU, LINK) + TILE, F32), pltpu.VMEM((STREAMS, 2, NU, LINK) + TILE, F32),
        pltpu.VMEM((STREAMS, NU) + PLANE + TILE, F32), pltpu.VMEM((STREAMS, NU, 4) + TILE, F32),
        pltpu.VMEM((STREAMS, 3, NU, 4) + TILE, F32), pltpu.VMEM((2, STREAMS, 3, NU) + TILE, F32),
        dma((STREAMS,)), dma((STREAMS, 2)), dma((3, STREAMS)), dma((3, STREAMS)),
    ]


def pick_block(ref, axis, b):
    return {"z": lambda: ref[b], "y": lambda: ref[:, b], "x": lambda: ref[:, :, b]}[axis]()


class Rings:
    def __init__(self, place, scratch, own, ready, done):
        self.p, self.own, self.ready, self.done = place, own, ready, done
        self.sent, self.got, self.t1, self.t2, self.d2, self.d3, self.ss, self.rs, self.ds, self.dr = scratch
        self.sent[:, :, FROM[1]:] = jnp.zeros((STREAMS, NU, LINK - FROM[1]) + TILE, F32)

    def links(self, e, par, link, lo):
        tiles = pl.ds(lo, LINK - lo)
        axis, way = UNITS[0 if link is None else link]
        at = slice(None) if link is None else link
        return pltpu.make_async_remote_copy(self.sent.at[e, at, tiles], self.got.at[e, par, at, tiles], self.ss.at[e], self.rs.at[e, par],
                                            device_id=self.p.neighbour("xyz"[axis], way), device_id_type=MESH)

    def wait(self, e, par, lo):
        c = self.links(e, par, None, lo)
        c.wait_send()
        c.wait_recv()

    def send(self, e, par, lo):
        for link in range(NU):
            self.links(e, par, link, lo).start()

    def link(self, u, phase):
        return (u + 2 * phase) % NU

    def came(self, e, par, u, phase):
        lo = FROM[phase]
        v = self.got[e, par, self.link(u, phase), lo:lo + HOP[phase]]
        return v.reshape((PLANE, PLANE[1:], ())[phase] + TILE)

    def go(self, e, u, phase, value):
        lo = FROM[phase]
        self.sent[e, self.link(u, phase), lo:lo + HOP[phase]] = value.reshape((HOP[phase],) + TILE)

    def block(self, u, phase, step):
        colour, way = UNITS[u]
        return self.p.block(AXES[colour][phase], way, step)

    def first(self, own, u, step):
        return pick_block(own.at[u], AXES[UNITS[u][0]][0], self.block(u, 0, step))

    def second_ref(self, e, u, b):
        order = AXES[UNITS[u][0]]
        rest = [a for a in NAT if a != order[0]]
        return self.t1.at[(e, u, slice(None), b) if rest.index(order[1]) == 1 else (e, u, b)]

    def second(self, e, u, step):
        return self.second_ref(e, u, self.block(u, 1, step))[...]

    def third(self, e, u, step):
        return self.t2[e, u, self.block(u, 2, step)]

    def straight(self, e, kind, u, j):
        phase = 1 if kind == 0 else 2
        axis = AXES[UNITS[u][0]][phase]
        b = lax.rem(self.p.at[axis] + j, QUAD)
        src = self.second_ref(e, u, b) if kind == 0 else self.t2.at[e, u, b]
        dst = self.landing(e, kind).at[j - 1, u]
        return pltpu.make_async_remote_copy(src, dst, self.ds.at[kind, e], self.dr.at[kind, e],
                                            device_id=self.p.neighbour(axis, j), device_id_type=MESH)

    def landing(self, e, kind):
        return self.d2.at[e] if kind == 0 else self.d3.at[kind - 1, e]

    def go_straight(self, e, kind):
        for j in (1, 3, 2):
            for u in range(NU):
                self.straight(e, kind, u, j).start()

    def wait_straight(self, e, kind):
        at = self.landing(e, kind)
        c = pltpu.make_async_remote_copy(at, at, self.ds.at[kind, e], self.dr.at[kind, e],
                                         device_id=self.p.neighbour("x", 1), device_id_type=MESH)
        c.wait_send()
        c.wait_recv()

    def sum_straight(self, e, kind, u):
        at = self.landing(e, kind)
        return at[0, u] + at[1, u] + at[2, u]

    def slot(self, s, step, drain=False):
        e = lax.rem(s, STREAMS)
        par = lax.rem(s // STREAMS, 2)
        old = 1 - par
        since = s - STREAMS * step
        chunk = lambda i: since // PERIOD - STREAMS * i
        live = lambda i: (since >= PERIOD * STREAMS * i) & (chunk(i) < CHUNKS)
        early = lambda i: chunk(i) < CHUNKS - 2 * STREAMS
        not_late = lambda i: chunk(i) < CHUNKS - STREAMS
        if not drain:
            early = not_late = lambda i: True
        both = lambda a, b: a if b is True else a & b
        ring1 = both(live(1), not_late(1))
        ring2 = both(live(2), early(2))
        late = live(1) & jnp.logical_not(not_late(1)) if drain else None
        middle = live(2) & not_late(2) & jnp.logical_not(early(2)) if drain else None
        if step == 0:
            was, more = live(1), both(live(2), not_late(2)) | both(live(3), early(3))
        else:
            was, more = live(0), ring1 | ring2

        @pl.when(was)
        def _():
            self.wait(e, old, 0)

        @pl.when(jnp.logical_not(was) & more)
        def _():
            self.wait(e, old, FROM[1])

        if step == 0:
            @pl.when(both(live(3), early(3)))
            def _():
                for u in range(NU):
                    self.done[chunk(3), u] = self.came(e, old, u, 2) + self.third(e, u, 3)

            @pl.when(both(live(2), not_late(2)))
            def _():
                for u in range(NU):
                    self.t2[e, u] = self.came(e, old, u, 1) + self.second(e, u, 3)
                    self.go(e, u, 2, self.third(e, u, 0))

            @pl.when(live(1))
            def _():
                own = self.own(chunk(1))
                for u in range(NU):
                    self.t1[e, u] = self.came(e, old, u, 0) + self.first(own, u, 3)
                    self.go(e, u, 1, self.second(e, u, 0))

            @pl.when(live(0))
            def _():
                self.ready(chunk(0))
                own = self.own(chunk(0))
                for u in range(NU):
                    self.go(e, u, 0, self.first(own, u, 0))
        else:
            @pl.when(ring2)
            def _():
                for u in range(NU):
                    self.go(e, u, 2, self.came(e, old, u, 2) + self.third(e, u, step))

            if drain and step == 1:
                @pl.when(middle)
                def _():
                    self.wait_straight(e, 2)
                    for u in range(NU):
                        self.done[chunk(2), u] = self.sum_straight(e, 2, u) + self.third(e, u, 3)

            @pl.when(ring1)
            def _():
                for u in range(NU):
                    self.go(e, u, 1, self.came(e, old, u, 1) + self.second(e, u, step))

            if drain:
                @pl.when(late)
                def _():
                    self.wait_straight(e, step - 1)
                    for u in range(NU):
                        if step == 1:
                            self.t2[e, u] = self.sum_straight(e, 0, u) + self.second(e, u, 3)
                        else:
                            self.done[chunk(1), u] = self.sum_straight(e, 1, u) + self.third(e, u, 3)

            @pl.when(live(0))
            def _():
                own = self.own(chunk(0))
                for u in range(NU):
                    self.go(e, u, 0, self.came(e, old, u, 0) + self.first(own, u, step))

        @pl.when(live(0))
        def _():
            self.send(e, par, 0)

        @pl.when(jnp.logical_not(live(0)) & (ring1 | ring2))
        def _():
            self.send(e, par, FROM[1])

        if drain and step < 2:
            @pl.when(late)
            def _():
                self.go_straight(e, step)

        if drain and step == 0:
            @pl.when(middle)
            def _():
                self.go_straight(e, 2)

    def step_of(self, s):
        return s * (STREAMS % PERIOD) % PERIOD if isinstance(s, int) else lax.rem(s * (STREAMS % PERIOD), PERIOD)

    def drain(self, start):
        def one(s, _):
            at = self.step_of(s)
            for step in range(PERIOD):
                @pl.when(at == step)
                def _():
                    self.slot(s, step, True)
            return 0

        lax.fori_loop(start, SLOTS - PERIOD + 5 * STREAMS + 1, one, 0)


def tiles_of_layer():
    down = [(3, g, j) for j in range(QUAD) for g in range(QUAD)]
    up = [(2, 0, j) for j in range(16)]
    out = [(1, 0, j) for j in range(QUAD)]
    qkv = [(0, 0, j) for j in range(12)]
    return down + up + out + qkv


TILES = tiles_of_layer()
PLACE_OF = {t: (i // 12, i % 12 // 6, i % 6) for i, t in enumerate(TILES)}


FWD_SEQS = 6
BWD_SEQS = 3
OWN_SLOTS = 7
SENT_SLOTS = 3
LEAD = 3
QKV_W, OUT_W, UP_W, DOWN_W = range(4)
HALF = 2 * D
PIECES = [(QKV_W, ()), (OUT_W, ()), (UP_W, (slice(None), pl.ds(0, HALF))), (DOWN_W, (pl.ds(0, HALF),)),
          (UP_W, (slice(None), pl.ds(HALF, HALF))), (DOWN_W, (pl.ds(HALF, HALF),))]
ALL = range(len(PIECES))
QKV_P, OUT_P, UP_P, DOWN_P = (0,), (1,), (2, 4), (3, 5)


def step_kernel(x, seed, wq, wo, wu, wd,
                y, rq, ro, ru, rd, hs, qs, ps, os, ms, us, es, out,
                grads, recv, done, h, qkv, p, o, m, u, e, g, g1, do, vq, vo, vu, vd,
                wsem, asem, gsem, psem, qsem, hsem, ysem, dsend, drecv, fsem, credit, wfree, *ring):
    place = Place()
    core = place.core
    partner = place.partner()
    mine = (wq, wo, wu, wd)
    theirs = (rq, ro, ru, rd)
    held = (vq, vo, vu, vd)
    acts = ((h, hs), (qkv, qs), (p, ps), (o, os), (m, ms), (u, us), (e, es))
    H, QKV, PROB, O, M, U, E = range(7)
    rows = pl.ds(core * ROWS, ROWS)

    def to_partner(src, dst, send, arrive):
        return pltpu.make_async_remote_copy(src, dst, send, arrive, device_id=partner, device_id_type=MESH)

    def piece_of(ref, i):
        at = PIECES[i][1]
        return ref.at[at] if at else ref

    def push(i, j):
        k = PIECES[i][0]
        return to_partner(piece_of(mine[k].at[j], i), piece_of(theirs[k].at[j], i), psem.at[i, j], qsem.at[i, j])

    def hand(i, l):
        k = PIECES[i][0]
        return to_partner(piece_of(mine[k].at[l], i), piece_of(held[k], i), hsem.at[0, i], hsem.at[1, i])

    def local_w(i, l, src):
        k = PIECES[i][0]
        return pltpu.make_async_copy(piece_of(src[k].at[lax.rem(l, 2)], i), piece_of(held[k], i), wsem.at[i])

    def fetch_w(i, l, arrives):
        @pl.when(l // 2 == core)
        def _():
            local_w(i, l, mine).start()

        @pl.when(l // 2 != core)
        def _():
            @pl.when(arrives)
            def _():
                push(i, lax.rem(l, 2)).wait_recv()
            local_w(i, l, theirs).start()

    def wait_w(*pieces):
        for i in pieces:
            local_w(i, 0, mine).wait()

    def act(i, l, back):
        vmem, hbm = acts[i]
        return pltpu.make_async_copy(hbm.at[l], vmem, asem.at[i]) if back else pltpu.make_async_copy(vmem, hbm.at[l], asem.at[i])

    def own_slot(chunk):
        return lax.rem(chunk, OWN_SLOTS)

    def sent_slot(chunk):
        return lax.rem(chunk, SENT_SLOTS)

    def cross(chunk):
        q = sent_slot(chunk)
        return to_partner(grads.at[OWN_SLOTS + q], recv.at[q], dsend.at[q], drecv.at[q])

    def ready(chunk):
        q = sent_slot(chunk)
        cross(chunk).wait_recv()
        for unit in range(NU):
            grads[own_slot(chunk), unit] = grads[own_slot(chunk), unit] + recv[q, unit]

        @pl.when(chunk + SENT_SLOTS < CHUNKS)
        def _():
            pl.semaphore_signal(credit.at[q], inc=1, device_id=partner, device_id_type=MESH)

    rings = Rings(place, ring, lambda chunk: grads.at[own_slot(chunk)], ready, done)

    x_in = pltpu.make_async_copy(x.at[rows], h, asem.at[H])
    x_in.start()
    seed_in = pltpu.make_async_copy(seed.at[rows], g, gsem)

    @pl.when(core == 0)
    def _():
        for i in ALL:
            local_w(i, 0, mine).start()
    greet([partner] + [place.neighbour(a, way) for a in NAT for way in (1, -1, 2)])

    @pl.when(core == 0)
    def _():
        for i in ALL:
            hand(i, 0).start()

    @pl.when(core == 1)
    def _():
        for j in range(2):
            for i in ALL:
                push(i, j).start()
    seed_in.start()
    x_in.wait()

    def layer(l, _):
        handed = (l < 2) & (core == 1)

        def weight(*pieces):
            @pl.when(jnp.logical_not(handed))
            def _():
                wait_w(*pieces)

            @pl.when(handed)
            def _():
                for i in pieces:
                    hand(i, 0).wait_recv()

        def used(group):
            @pl.when((l == 0) & (core == 1))
            def _():
                pl.semaphore_signal(wfree.at[group], inc=1, device_id=partner, device_id_type=MESH)

        def hand_on(at, group, *pieces):
            @pl.when((l == at) & (core == 0))
            def _():
                pl.semaphore_wait(wfree.at[group], 1)
                for i in pieces:
                    hand(i, 0).wait_send()
                    hand(i, 1).start()

        def again(i):
            @pl.when(l > 0)
            def _():
                act(i, l - 1, False).wait()

        def save(i):
            @pl.when(l < LAYERS - 1)
            def _():
                act(i, l, False).start()

        def next_w(when, to, *pieces):
            @pl.when(when)
            def _():
                for i in pieces:
                    fetch_w(i, to, True)

        more = l < LAYERS - 1
        again(H)

        @pl.when(l > 0)
        def _():
            h[...] = do[...]
        save(H)
        weight(0)
        again(QKV)
        hf = h[...].astype(F32)
        qkv[...] = dot((hf * inv_rms(hf)).astype(BF16), vq[...]).astype(BF16)
        used(0)
        save(QKV)
        again(PROB)
        again(O)

        for i in range(NSEQ // FWD_SEQS):
            attention_fwd(i, FWD_SEQS, qkv, p, o)
        hand_on(0, 0, 0)
        hand_on(1, 3, 4, 5)
        save(PROB)
        save(O)
        weight(1)
        again(M)
        mb = (h[...].astype(F32) + dot(o[...], vo[...])).astype(BF16)
        m[...] = mb
        mf = mb.astype(F32)
        g1[...] = (mf * inv_rms(mf)).astype(BF16)
        used(1)
        save(M)
        again(U)
        again(E)
        weight(2, 3)

        def mlp(j):
            cols = slice(j * HALF, (j + 1) * HALF)
            ub = dot(g1[...], vu[:, cols]).astype(BF16)
            u[:, cols] = ub
            eb = gelu(ub.astype(F32)).astype(BF16)
            e[:, cols] = eb
            return dot(eb, vd[cols, :])

        half_way = m[...].astype(F32) + mlp(0)
        for unit in range(NU):
            for col in range(QUAD):
                grads[0, unit, :, :, col] = half_way[unit * SEQ:unit * SEQ + SEQ, col * LN:col * LN + LN].reshape(PLANE + TILE)
        used(2)
        hand_on(0, 1, 1)
        mine_next = more & jnp.logical_or(l > 0, core == 0)
        next_w(mine_next, l + 1, 0, 1)
        weight(4, 5)
        rest = mlp(1)
        for unit in range(NU):
            part = pl.ds(unit * SEQ, SEQ)
            for col in range(QUAD):
                cols = slice(col * LN, col * LN + LN)
                do[part, cols] = (grads[0, unit, :, :, col].reshape((SEQ, LN)) + rest[unit * SEQ:unit * SEQ + SEQ, cols]).astype(BF16)
        used(3)
        hand_on(0, 2, 2, 3)
        next_w(mine_next, l + 1, 2, 3, 4, 5)

        @pl.when((l == 1) & (core == 0))
        def _():
            for j in (1, 0):
                for i in ALL:
                    push(i, j).start()
        save(U)
        save(E)
        return 0

    lax.fori_loop(0, LAYERS, layer, 0)
    y_here = pltpu.make_async_copy(do, y.at[rows], ysem.at[0])
    y_there = to_partner(do, y.at[rows], ysem.at[1], ysem.at[2])
    y_here.start()
    y_there.start()

    def free(chunk):
        @pl.when(chunk >= SENT_SLOTS)
        def _():
            cross(chunk).wait_send()

    def put(base, tile, value):
        q, half, unit = PLACE_OF[tile]
        index = jnp.where(core == half, own_slot(base + q), OWN_SLOTS + sent_slot(base + q))
        grads[index, unit] = value.reshape(CUBE + TILE)

    def ship(chunk):
        @pl.when(chunk >= SENT_SLOTS)
        def _():
            pl.semaphore_wait(credit.at[sent_slot(chunk)], 1)
        cross(chunk).start()

    def down_grad(base, halves):
        for half in halves:
            if half == 0:
                free(base)
                free(base + 1)
            w = dot_first(e[...], g[:, half * 256:half * 256 + 256]).reshape((64, QUAD, 8, 256))
            for j in range(2):
                for rg in range(QUAD):
                    put(base, (DOWN_W, rg, 2 * half + j), w[:, rg, :, j * LN:j * LN + LN])
            if half == 1:
                ship(base)

    def gelu_part(lo, hi):
        de = dot_last(g[...], vd[lo:hi, :])
        u[:, lo:hi] = (gelu_slope(u[:, lo:hi].astype(F32)) * de).astype(BF16)

    def wide_grad(base, array, a, b, parts):
        for part in parts:
            w = dot_first(a, b[:, part * D:part * D + D]).reshape((64, 8, D))
            for j in range(QUAD):
                put(base, (array, 0, QUAD * part + j), w[:, :, j * LN:j * LN + LN])

    seed_in.wait()
    down_grad(0, range(2))
    act(E, LAYERS - 2, True).start()
    y_here.wait()
    y_there.wait_send()

    def iteration(it, _):
        l = LAYERS - 1 - it
        more = it < LAYERS - 1
        base = 4 * it

        def loaded(acts_of, pieces=()):
            @pl.when(it > 0)
            def _():
                for i in acts_of:
                    act(i, l, True).wait()
                wait_w(*pieces)

        def after(acts_of, pieces=()):
            @pl.when(more)
            def _():
                for i in pieces:
                    fetch_w(i, l - 1, l <= 2)
                for i in acts_of:
                    act(i, l - 1, True).start()

        def piece(n):
            if n == 0:
                loaded((U,), DOWN_P)
                gelu_part(0, 3 * 256)
            elif n == 1:
                gelu_part(3 * 256, 3 * D)
            elif n == 2:
                gelu_part(3 * D, QUAD * D)
                after((), DOWN_P)
                loaded((M,))
                mf = m[...].astype(F32)
                g1[...] = (mf * inv_rms(mf)).astype(BF16)
                wide_grad(base, UP_W, g1[...], u, (0,))
            elif n == 3:
                free(base + 2)
                wide_grad(base, UP_W, g1[...], u, (1, 2, 3))
                ship(base + 1)
            elif n == 4:
                loaded((), UP_P)
                dc = dot_last(u[...], vu[...])
                g1[...] = (g[...].astype(F32) + rms_bwd(m[...].astype(F32), dc)).astype(BF16)
                after((U, M), UP_P)
            elif n == 5:
                loaded((O,), OUT_P)
                do[...] = dot_last(g1[...], vo[...]).astype(BF16)
                wide_grad(base, OUT_W, o[...], g1, (0,))
                ship(base + 2)
                after((O,), OUT_P)
            elif n in (6, 7):
                if n == 6:
                    loaded((PROB, QKV))
                attention_bwd(n - 6, BWD_SEQS, qkv, p, do)
                if n == 7:
                    after((PROB,))
            elif n == 8:
                loaded((H,))
                free(base + 3)
                hf = h[...].astype(F32)
                wide_grad(base, QKV_W, (hf * inv_rms(hf)).astype(BF16), qkv, range(3))
                ship(base + 3)
            elif n == 9:
                loaded((), QKV_P)
                da = dot_last(qkv[...], vq[...])
                g[...] = (g1[...].astype(F32) + rms_bwd(h[...].astype(F32), da)).astype(BF16)
                after((H, QKV), QKV_P)
            else:
                @pl.when(more)
                def _():
                    if n == 10:
                        act(E, l - 1, True).wait()
                    down_grad(base + QUAD, (n - 10,))

                if n == 11:
                    @pl.when(l > 1)
                    def _():
                        act(E, l - 2, True).start()

        for n in range(12):
            s = 12 * it + n - LEAD
            step = rings.step_of(n + 2 * PERIOD - LEAD)
            if n < LEAD:
                @pl.when(it > 0)
                def _():
                    rings.slot(s, step)
            else:
                rings.slot(s, step)
            piece(n)
        return 0

    lax.fori_loop(0, LAYERS, iteration, 0)
    rings.drain(SLOTS - LEAD)

    for q in range(SENT_SLOTS):
        cross(q).wait_send()
    last = to_partner(done.at[pl.ds(8 * core, 8)], out.at[core], fsem.at[0], fsem.at[1])
    last.start()
    kept = pltpu.make_async_copy(done.at[pl.ds(8 * (1 - core), 8)], out.at[core], gsem)
    kept.start()
    for j in range(2):
        for i in ALL:
            push(i, j).wait_send()

    @pl.when(core == 0)
    def _():
        for i in ALL:
            hand(i, 0).wait_send()
    y_there.wait_recv()
    kept.wait()
    last.wait_send()
    last.wait_recv()


def train_step(x, seed, weights):
    anywhere = pl.BlockSpec(memory_space=pl.ANY)
    dma = pltpu.SemaphoreType.DMA
    act = lambda cols, dt=BF16: pltpu.VMEM((ROWS, cols), dt)
    saved = lambda cols, dt=BF16: jax.ShapeDtypeStruct((LAYERS - 1, ROWS, cols), dt)
    outs = pl.pallas_call(
        step_kernel,
        name="step",
        out_shape=[jax.ShapeDtypeStruct((2 * ROWS, D), BF16)] + [jax.ShapeDtypeStruct((2,) + s, BF16) for s in W_SHAPES]
        + [saved(D), saved(3 * D), saved(2 * D, F32), saved(D), saved(D), saved(QUAD * D), saved(QUAD * D)]
        + [jax.ShapeDtypeStruct((2, 8, NU) + TILE, F32)],
        in_specs=[anywhere] * 6,
        out_specs=[anywhere] * 13,
        scratch_shapes=[
            pltpu.VMEM((OWN_SLOTS + SENT_SLOTS, NU) + CUBE + TILE, F32),
            pltpu.VMEM((SENT_SLOTS, NU) + CUBE + TILE, F32),
            pltpu.VMEM((CHUNKS, NU) + TILE, F32),
            act(D), act(3 * D), act(2 * D, F32), act(D), act(D), act(QUAD * D), act(QUAD * D), act(D), act(D), act(D),
        ] + [pltpu.VMEM(s, BF16) for s in W_SHAPES] + [
            dma((6,)), dma((7,)), dma, dma((6, 2)), dma((6, 2)), dma((2, 6)), dma((3,)), dma((QUAD,)), dma((QUAD,)), dma((2,)),
            pltpu.SemaphoreType.REGULAR((QUAD,)), pltpu.SemaphoreType.REGULAR((QUAD,)),
        ] + ring_scratch(),
        compiler_params=pltpu.CompilerParams(collective_id=1, has_side_effects=True, vmem_limit_bytes=67043328),
    )(x, seed, *weights)
    return outs[0], outs[-1]


ROW_SHAPES = ((2, 8, 3 * D), (2, 8, D), (2, 8, QUAD * D), (2, 32, D))


def finish_kernel(y_in, sums_in, y, gq, go, gu, gd, buf, sums, bq, bo, bu, bd, in_sem, out_sem, sum_sem, grad_sem):
    parts = buf.shape[0]
    here = pltpu.make_async_copy(sums_in, sums, sum_sem)
    here.start()
    into = [pltpu.make_async_copy(y_in.at[i], buf.at[i], in_sem.at[i]) for i in range(parts)]
    out = [pltpu.make_async_copy(buf.at[i], y.at[i], out_sem.at[i]) for i in range(parts)]
    for c in into:
        c.start()
    here.wait()
    rows = (bq, bo, bu, bd)
    for layer in range(2):
        for tile in TILES:
            array, rg, col = tile
            q, half, unit = PLACE_OF[tile]
            rows[array][layer, rg * 8:rg * 8 + 8, col * LN:col * LN + LN] = sums[half, QUAD * (1 - layer) + q, unit]
    out += [pltpu.make_async_copy(r, o, grad_sem.at[i]) for i, (r, o) in enumerate(zip(rows, (gq, go, gu, gd)))]
    for c, d in zip(into, out):
        c.wait()
        d.start()
    for d in out[parts:]:
        d.start()
    for d in out:
        d.wait()


def finish(y, sums, parts=6):
    anywhere = pl.BlockSpec(memory_space=pl.ANY)
    dma = pltpu.SemaphoreType.DMA
    shape = (parts, 2 * ROWS // parts, D)
    return pl.pallas_call(
        finish_kernel,
        name="finish",
        out_shape=[jax.ShapeDtypeStruct(shape, BF16)] + [jax.ShapeDtypeStruct(s, F32) for s in ROW_SHAPES],
        in_specs=[anywhere] * 2,
        out_specs=[anywhere] * 5,
        scratch_shapes=[pltpu.VMEM(shape, BF16), pltpu.VMEM(sums.shape, F32)] + [pltpu.VMEM(s, F32) for s in ROW_SHAPES]
        + [dma((parts,)), dma((parts,)), dma, dma((QUAD,))],
    )(y.reshape(shape), sums)


def solution(mesh):
    def step(x_in, seed_grad, w_qkv, w_out, w_up, w_down):
        shape = x_in.shape
        weights = (w_qkv, w_out, w_up, w_down)
        y, sums = train_step(x_in.reshape(2 * ROWS, D), seed_grad.reshape(2 * ROWS, D), weights)
        y, *grads = finish(y, sums)
        return y.reshape(shape), *grads

    act, weight, grad = P(None, "dp"), P("pp"), P("pp", "dp")
    return jax.shard_map(
        step,
        mesh=mesh,
        in_specs=(act, act, weight, weight, weight, weight),
        out_specs=(act, grad, grad, grad, grad),
        check_vma=False,
    )
```

```python
import functools
import math

import jax
import jax.numpy as jnp
from jax import lax
from jax.experimental import pallas as pl
from jax.experimental.pallas import tpu as pltpu
from jax.sharding import PartitionSpec as P

F32 = jnp.float32
BF16 = jnp.bfloat16
MESH = pl.DeviceIdType.MESH

D = 512
HD = 64
LN = 128
TILE = (8, LN)
QUAD = 4
PLANE = (QUAD, QUAD)
CUBE = PLANE + (QUAD,)
NU = 6
SEQ = LN
NSEQ = 6
ROWS = NSEQ * SEQ
LAYERS = 4
EPS = 1e-6
GELU_C1 = math.sqrt(2.0 / math.pi)
GELU_C2 = GELU_C1 * 0.044715
EXP2_SCALE = HD ** -0.5 * math.log2(math.e)
W_SHAPES = ((D, 3 * D), (D, D), (D, QUAD * D), (QUAD * D, D))
LAST = (((1,), (1,)), ((), ()))
FIRST = (((0,), (0,)), ((), ()))


def dot(a, b):
    return jnp.dot(a, b, preferred_element_type=F32)


def dot_last(a, b):
    return lax.dot_general(a, b, LAST, preferred_element_type=F32)


def dot_first(a, b):
    return lax.dot_general(a, b, FIRST, preferred_element_type=F32)


def inv_rms(h):
    return lax.rsqrt(jnp.mean(h * h, axis=-1, keepdims=True) + EPS)


def rms_bwd(h, g):
    ir = inv_rms(h)
    n = h * ir
    return ir * (g - n * jnp.mean(g * n, axis=-1, keepdims=True))


def gelu(u):
    t = jnp.tanh(u * (GELU_C1 + GELU_C2 * (u * u)))
    return u * (0.5 * t + 0.5)


def gelu_slope(u):
    a = GELU_C2 * (u * u)
    t = jnp.tanh(u * (a + GELU_C1))
    half = 0.5 * t + 0.5
    return half + u * half * (1.0 - t) * (3.0 * a + GELU_C1)


def block_diag(x):
    first = lax.broadcasted_iota(jnp.int32, (SEQ, 2 * HD), 1) < HD
    zero = jnp.zeros_like(x)
    return jnp.concatenate([jnp.where(first, x, zero), jnp.where(first, zero, x)], axis=0)


def units_of(step, n_seqs):
    return [(pl.ds(pl.multiple_of((step * n_seqs + n) * SEQ, SEQ), SEQ), pair) for n in range(n_seqs) for pair in range(QUAD)]


def attention_fwd(step, n_seqs, qkv, p_out, o_out):
    key = lax.broadcasted_iota(jnp.int32, (SEQ, SEQ), 0)
    query = lax.broadcasted_iota(jnp.int32, (SEQ, SEQ), 1)
    allowed = key <= query
    units = units_of(step, n_seqs)

    def scores(rows, pair):
        c = pair * LN
        return dot_last(qkv[rows, D + c:D + c + LN], block_diag(qkv[rows, c:c + LN]))

    ahead = 2
    pending = [scores(*u) for u in units[:ahead]]
    for i, (rows, pair) in enumerate(units):
        if i + ahead < len(units):
            pending.append(scores(*units[i + ahead]))
        s = pending[i]
        c = pair * LN
        probs = []
        for head in range(2):
            sh = jnp.where(allowed, s[:, head * LN:head * LN + LN], -1e30)
            e = jnp.exp2((sh - jnp.max(sh, axis=0, keepdims=True)) * EXP2_SCALE)
            p = e * (1.0 / jnp.sum(e, axis=0, keepdims=True))
            p_out[rows, 2 * c + head * LN:2 * c + head * LN + LN] = p
            probs.append(p.astype(BF16))
        v = qkv[rows, 2 * D + c:2 * D + c + LN]
        o_out[rows, c:c + LN] = dot_first(jnp.concatenate(probs, axis=0), block_diag(v)).astype(BF16)


def attention_bwd(step, n_seqs, qkv, p_in, do):
    units = units_of(step, n_seqs)

    def first(rows, pair):
        c = pair * LN
        d = block_diag(do[rows, c:c + LN])
        return d, dot_last(qkv[rows, 2 * D + c:2 * D + c + LN], d)

    ahead = 2
    pending = [first(*u) for u in units[:ahead]]
    for i, (rows, pair) in enumerate(units):
        if i + ahead < len(units):
            pending.append(first(*units[i + ahead]))
        d, dp = pending[i]
        c = pair * LN
        q = qkv[rows, c:c + LN]
        k = qkv[rows, D + c:D + c + LN]
        p = p_in[rows, 2 * c:2 * c + 256]
        dv = dot(p.astype(BF16), d).astype(BF16)
        pd = p * dp
        ds = ((pd - p * jnp.sum(pd, axis=0, keepdims=True)) * HD ** -0.5).astype(BF16)
        dk = dot(ds, block_diag(q)).astype(BF16)
        dq = dot_first(jnp.concatenate([ds[:, :LN], ds[:, LN:]], axis=0), block_diag(k)).astype(BF16)
        qkv[rows, c:c + LN] = dq
        qkv[rows, D + c:D + c + LN] = dk
        qkv[rows, 2 * D + c:2 * D + c + LN] = dv


AXES = (("x", "y", "z"), ("y", "z", "x"), ("z", "x", "y"))
NAT = ("z", "y", "x")
STRIDE = {"x": 1, "y": 4, "z": 16}
UNITS = [(colour, way) for colour in range(3) for way in (1, -1)]


class Place:
    def __init__(self):
        self.core = lax.axis_index("pp")
        self.dp = lax.axis_index("dp")
        self.at = {"x": lax.rem(self.dp, QUAD), "y": lax.rem(self.dp // QUAD, QUAD), "z": self.dp // 16}

    def neighbour(self, axis, way):
        c = self.at[axis]
        return (self.core, self.dp + (lax.rem(c + way + QUAD, QUAD) - c) * STRIDE[axis])

    def partner(self):
        return (1 - self.core, self.dp)

    def block(self, axis, way, step):
        return lax.rem(self.at[axis] - way * (1 + step) + 8, QUAD)


def greet(peers):
    barrier = pltpu.get_barrier_semaphore()
    for p in peers:
        pl.semaphore_signal(barrier, inc=1, device_id=p, device_id_type=MESH)
    pl.semaphore_wait(barrier, len(peers))


CHUNKS = 16
PERIOD = 3
STREAMS = 4
SLOTS = PERIOD * CHUNKS
HOP = (16, 4, 1)
FROM = (0, 16, 20)
LINK = 21


def ring_scratch():
    dma = pltpu.SemaphoreType.DMA
    return [
        pltpu.VMEM((STREAMS, NU, LINK) + TILE, F32), pltpu.VMEM((STREAMS, 2, NU, LINK) + TILE, F32),
        pltpu.VMEM((STREAMS, NU) + PLANE + TILE, F32), pltpu.VMEM((STREAMS, NU, 4) + TILE, F32),
        pltpu.VMEM((STREAMS, 3, NU, 4) + TILE, F32), pltpu.VMEM((2, STREAMS, 3, NU) + TILE, F32),
        dma((STREAMS,)), dma((STREAMS, 2)), dma((3, STREAMS)), dma((3, STREAMS)),
    ]


def pick_block(ref, axis, b):
    return {"z": lambda: ref[b], "y": lambda: ref[:, b], "x": lambda: ref[:, :, b]}[axis]()


class Rings:
    def __init__(self, place, scratch, own, ready, done):
        self.p, self.own, self.ready, self.done = place, own, ready, done
        self.sent, self.got, self.t1, self.t2, self.d2, self.d3, self.ss, self.rs, self.ds, self.dr = scratch
        self.sent[:, :, FROM[1]:] = jnp.zeros((STREAMS, NU, LINK - FROM[1]) + TILE, F32)

    def links(self, e, par, link, lo):
        tiles = pl.ds(lo, LINK - lo)
        axis, way = UNITS[0 if link is None else link]
        at = slice(None) if link is None else link
        return pltpu.make_async_remote_copy(self.sent.at[e, at, tiles], self.got.at[e, par, at, tiles], self.ss.at[e], self.rs.at[e, par],
                                            device_id=self.p.neighbour("xyz"[axis], way), device_id_type=MESH)

    def wait(self, e, par, lo):
        c = self.links(e, par, None, lo)
        c.wait_send()
        c.wait_recv()

    def send(self, e, par, lo):
        for link in range(NU):
            self.links(e, par, link, lo).start()

    def link(self, u, phase):
        return (u + 2 * phase) % NU

    def came(self, e, par, u, phase):
        lo = FROM[phase]
        v = self.got[e, par, self.link(u, phase), lo:lo + HOP[phase]]
        return v.reshape((PLANE, PLANE[1:], ())[phase] + TILE)

    def go(self, e, u, phase, value):
        lo = FROM[phase]
        self.sent[e, self.link(u, phase), lo:lo + HOP[phase]] = value.reshape((HOP[phase],) + TILE)

    def block(self, u, phase, step):
        colour, way = UNITS[u]
        return self.p.block(AXES[colour][phase], way, step)

    def first(self, own, u, step):
        return pick_block(own.at[u], AXES[UNITS[u][0]][0], self.block(u, 0, step))

    def second_ref(self, e, u, b):
        order = AXES[UNITS[u][0]]
        rest = [a for a in NAT if a != order[0]]
        return self.t1.at[(e, u, slice(None), b) if rest.index(order[1]) == 1 else (e, u, b)]

    def second(self, e, u, step):
        return self.second_ref(e, u, self.block(u, 1, step))[...]

    def third(self, e, u, step):
        return self.t2[e, u, self.block(u, 2, step)]

    def straight(self, e, kind, u, j):
        phase = 1 if kind == 0 else 2
        axis = AXES[UNITS[u][0]][phase]
        b = lax.rem(self.p.at[axis] + j, QUAD)
        src = self.second_ref(e, u, b) if kind == 0 else self.t2.at[e, u, b]
        dst = self.landing(e, kind).at[j - 1, u]
        return pltpu.make_async_remote_copy(src, dst, self.ds.at[kind, e], self.dr.at[kind, e],
                                            device_id=self.p.neighbour(axis, j), device_id_type=MESH)

    def landing(self, e, kind):
        return self.d2.at[e] if kind == 0 else self.d3.at[kind - 1, e]

    def go_straight(self, e, kind):
        for j in (2, 1, 3):
            for u in range(NU):
                self.straight(e, kind, u, j).start()

    def wait_straight(self, e, kind):
        at = self.landing(e, kind)
        c = pltpu.make_async_remote_copy(at, at, self.ds.at[kind, e], self.dr.at[kind, e],
                                         device_id=self.p.neighbour("x", 1), device_id_type=MESH)
        c.wait_send()
        c.wait_recv()

    def sum_straight(self, e, kind, u):
        at = self.landing(e, kind)
        return at[0, u] + at[1, u] + at[2, u]

    def slot(self, s, step, drain=False):
        e = lax.rem(s, STREAMS)
        par = lax.rem(s // STREAMS, 2)
        old = 1 - par
        since = s - STREAMS * step
        chunk = lambda i: since // PERIOD - STREAMS * i
        live = lambda i: (since >= PERIOD * STREAMS * i) & (chunk(i) < CHUNKS)
        early = lambda i: chunk(i) < CHUNKS - 2 * STREAMS
        not_late = lambda i: chunk(i) < CHUNKS - STREAMS
        if not drain:
            early = not_late = lambda i: True
        both = lambda a, b: a if b is True else a & b
        ring1 = both(live(1), not_late(1))
        ring2 = both(live(2), early(2))
        late = live(1) & jnp.logical_not(not_late(1)) if drain else None
        middle = live(2) & not_late(2) & jnp.logical_not(early(2)) if drain else None
        if step == 0:
            was, more = live(1), both(live(2), not_late(2)) | both(live(3), early(3))
        else:
            was, more = live(0), ring1 | ring2

        @pl.when(was)
        def _():
            self.wait(e, old, 0)

        @pl.when(jnp.logical_not(was) & more)
        def _():
            self.wait(e, old, FROM[1])

        if step == 0:
            @pl.when(both(live(3), early(3)))
            def _():
                for u in range(NU):
                    self.done[chunk(3), u] = self.came(e, old, u, 2) + self.third(e, u, 3)

            @pl.when(both(live(2), not_late(2)))
            def _():
                for u in range(NU):
                    self.t2[e, u] = self.came(e, old, u, 1) + self.second(e, u, 3)
                    self.go(e, u, 2, self.third(e, u, 0))

            @pl.when(live(1))
            def _():
                own = self.own(chunk(1))
                for u in range(NU):
                    self.t1[e, u] = self.came(e, old, u, 0) + self.first(own, u, 3)
                    self.go(e, u, 1, self.second(e, u, 0))

            @pl.when(live(0))
            def _():
                self.ready(chunk(0))
                own = self.own(chunk(0))
                for u in range(NU):
                    self.go(e, u, 0, self.first(own, u, 0))
        else:
            @pl.when(ring2)
            def _():
                for u in range(NU):
                    self.go(e, u, 2, self.came(e, old, u, 2) + self.third(e, u, step))

            if drain and step == 1:
                @pl.when(middle)
                def _():
                    self.wait_straight(e, 2)
                    for u in range(NU):
                        self.done[chunk(2), u] = self.sum_straight(e, 2, u) + self.third(e, u, 3)

            @pl.when(ring1)
            def _():
                for u in range(NU):
                    self.go(e, u, 1, self.came(e, old, u, 1) + self.second(e, u, step))

            if drain:
                @pl.when(late)
                def _():
                    self.wait_straight(e, step - 1)
                    for u in range(NU):
                        if step == 1:
                            self.t2[e, u] = self.sum_straight(e, 0, u) + self.second(e, u, 3)
                        else:
                            self.done[chunk(1), u] = self.sum_straight(e, 1, u) + self.third(e, u, 3)

            @pl.when(live(0))
            def _():
                own = self.own(chunk(0))
                for u in range(NU):
                    self.go(e, u, 0, self.came(e, old, u, 0) + self.first(own, u, step))

        @pl.when(live(0))
        def _():
            self.send(e, par, 0)

        @pl.when(jnp.logical_not(live(0)) & (ring1 | ring2))
        def _():
            self.send(e, par, FROM[1])

        if drain and step < 2:
            @pl.when(late)
            def _():
                self.go_straight(e, step)

        if drain and step == 0:
            @pl.when(middle)
            def _():
                self.go_straight(e, 2)

    def step_of(self, s):
        return s * (STREAMS % PERIOD) % PERIOD if isinstance(s, int) else lax.rem(s * (STREAMS % PERIOD), PERIOD)

    def drain(self, start):
        def one(s, _):
            at = self.step_of(s)
            for step in range(PERIOD):
                @pl.when(at == step)
                def _():
                    self.slot(s, step, True)
            return 0

        lax.fori_loop(start, SLOTS - PERIOD + 5 * STREAMS + 1, one, 0)


def tiles_of_layer():
    down = [(3, g, j) for j in range(QUAD) for g in range(QUAD)]
    up = [(2, 0, j) for j in range(16)]
    out = [(1, 0, j) for j in range(QUAD)]
    qkv = [(0, 0, j) for j in range(12)]
    return down + up + out + qkv


TILES = tiles_of_layer()
PLACE_OF = {t: (i // 12, i % 12 // 6, i % 6) for i, t in enumerate(TILES)}


BWD_SEQS = 3
OWN_SLOTS = 7
SENT_SLOTS = 3
LEAD = 3
QKV_W, OUT_W, UP_W, DOWN_W = range(4)
HALF = 2 * D
PIECES = [(QKV_W, ()), (OUT_W, ()), (UP_W, (slice(None), pl.ds(0, HALF))), (DOWN_W, (pl.ds(0, HALF),)),
          (UP_W, (slice(None), pl.ds(HALF, HALF))), (DOWN_W, (pl.ds(HALF, HALF),))]
ALL = range(len(PIECES))
QKV_P, OUT_P, UP_P, DOWN_P = (0,), (1,), (2, 4), (3, 5)


def step_kernel(x, seed, wq, wo, wu, wd,
                y, rq, ro, ru, rd, hs, qs, ps, os, ms, us, es, out,
                grads, recv, done, h, qkv, p, o, m, u, e, g, g1, do, vq, vo, vu, vd,
                wsem, asem, gsem, psem, qsem, hsem, ysem, dsend, drecv, fsem, credit, wfree, *ring):
    place = Place()
    core = place.core
    partner = place.partner()
    mine = (wq, wo, wu, wd)
    theirs = (rq, ro, ru, rd)
    held = (vq, vo, vu, vd)
    acts = ((h, hs), (qkv, qs), (p, ps), (o, os), (m, ms), (u, us), (e, es))
    H, QKV, PROB, O, M, U, E = range(7)
    rows = pl.ds(core * ROWS, ROWS)

    def to_partner(src, dst, send, arrive):
        return pltpu.make_async_remote_copy(src, dst, send, arrive, device_id=partner, device_id_type=MESH)

    def piece_of(ref, i):
        at = PIECES[i][1]
        return ref.at[at] if at else ref

    def push(i, j):
        k = PIECES[i][0]
        return to_partner(piece_of(mine[k].at[j], i), piece_of(theirs[k].at[j], i), psem.at[i, j], qsem.at[i, j])

    def hand(i, l):
        k = PIECES[i][0]
        return to_partner(piece_of(mine[k].at[l], i), piece_of(held[k], i), hsem.at[0, i], hsem.at[1, i])

    def local_w(i, l, src):
        k = PIECES[i][0]
        return pltpu.make_async_copy(piece_of(src[k].at[lax.rem(l, 2)], i), piece_of(held[k], i), wsem.at[i])

    def fetch_w(i, l, arrives):
        @pl.when(l // 2 == core)
        def _():
            local_w(i, l, mine).start()

        @pl.when(l // 2 != core)
        def _():
            @pl.when(arrives)
            def _():
                push(i, lax.rem(l, 2)).wait_recv()
            local_w(i, l, theirs).start()

    def wait_w(*pieces):
        for i in pieces:
            local_w(i, 0, mine).wait()

    def act(i, l, back):
        vmem, hbm = acts[i]
        return pltpu.make_async_copy(hbm.at[l], vmem, asem.at[i]) if back else pltpu.make_async_copy(vmem, hbm.at[l], asem.at[i])

    def own_slot(chunk):
        return lax.rem(chunk, OWN_SLOTS)

    def sent_slot(chunk):
        return lax.rem(chunk, SENT_SLOTS)

    def cross(chunk):
        q = sent_slot(chunk)
        return to_partner(grads.at[OWN_SLOTS + q], recv.at[q], dsend.at[q], drecv.at[q])

    def ready(chunk):
        q = sent_slot(chunk)
        cross(chunk).wait_recv()
        for unit in range(NU):
            grads[own_slot(chunk), unit] = grads[own_slot(chunk), unit] + recv[q, unit]

        @pl.when(chunk + SENT_SLOTS < CHUNKS)
        def _():
            pl.semaphore_signal(credit.at[q], inc=1, device_id=partner, device_id_type=MESH)

    rings = Rings(place, ring, lambda chunk: grads.at[own_slot(chunk)], ready, done)

    x_in = pltpu.make_async_copy(x.at[rows], h, asem.at[H])
    x_in.start()
    seed_in = pltpu.make_async_copy(seed.at[rows], g, gsem)

    @pl.when(core == 0)
    def _():
        for i in ALL:
            local_w(i, 0, mine).start()
    greet([partner] + [place.neighbour(a, way) for a in NAT for way in (1, -1, 2)])

    @pl.when(core == 0)
    def _():
        for i in ALL:
            hand(i, 0).start()

    @pl.when(core == 1)
    def _():
        for j in range(2):
            for i in ALL:
                push(i, j).start()
    seed_in.start()
    x_in.wait()

    def layer(l, _):
        handed = (l < 2) & (core == 1)

        def weight(*pieces):
            @pl.when(jnp.logical_not(handed))
            def _():
                wait_w(*pieces)

            @pl.when(handed)
            def _():
                for i in pieces:
                    hand(i, 0).wait_recv()

        def used(group):
            @pl.when((l == 0) & (core == 1))
            def _():
                pl.semaphore_signal(wfree.at[group], inc=1, device_id=partner, device_id_type=MESH)

        def hand_on(at, group, *pieces):
            @pl.when((l == at) & (core == 0))
            def _():
                pl.semaphore_wait(wfree.at[group], 1)
                for i in pieces:
                    hand(i, 0).wait_send()
                    hand(i, 1).start()

        def again(i):
            @pl.when(l > 0)
            def _():
                act(i, l - 1, False).wait()

        def save(i):
            @pl.when(l < LAYERS - 1)
            def _():
                act(i, l, False).start()

        def next_w(when, to, *pieces):
            @pl.when(when)
            def _():
                for i in pieces:
                    fetch_w(i, to, True)

        more = l < LAYERS - 1
        again(H)

        @pl.when(l > 0)
        def _():
            h[...] = do[...]
        save(H)
        weight(0)
        for i in (QKV, PROB, O):
            again(i)
        hf = h[...].astype(F32)
        qkv[...] = dot((hf * inv_rms(hf)).astype(BF16), vq[...]).astype(BF16)
        attention_fwd(0, NSEQ, qkv, p, o)
        used(0)
        hand_on(0, 0, 0)
        hand_on(1, 3, 4, 5)
        for i in (QKV, PROB, O):
            save(i)
        weight(1)
        again(M)
        mb = (h[...].astype(F32) + dot(o[...], vo[...])).astype(BF16)
        m[...] = mb
        mf = mb.astype(F32)
        g1[...] = (mf * inv_rms(mf)).astype(BF16)
        used(1)
        save(M)
        again(U)
        again(E)
        weight(2, 3)

        def mlp(j):
            cols = slice(j * HALF, (j + 1) * HALF)
            ub = dot(g1[...], vu[:, cols]).astype(BF16)
            u[:, cols] = ub
            eb = gelu(ub.astype(F32)).astype(BF16)
            e[:, cols] = eb
            return dot(eb, vd[cols, :])

        half_way = m[...].astype(F32) + mlp(0)
        for unit in range(NU):
            for col in range(QUAD):
                grads[0, unit, :, :, col] = half_way[unit * SEQ:unit * SEQ + SEQ, col * LN:col * LN + LN].reshape(PLANE + TILE)
        used(2)
        hand_on(0, 1, 1)
        mine_next = more & jnp.logical_or(l > 0, core == 0)
        next_w(mine_next, l + 1, 0, 1)
        weight(4, 5)
        rest = mlp(1)
        for unit in range(NU):
            part = pl.ds(unit * SEQ, SEQ)
            for col in range(QUAD):
                cols = slice(col * LN, col * LN + LN)
                do[part, cols] = (grads[0, unit, :, :, col].reshape((SEQ, LN)) + rest[unit * SEQ:unit * SEQ + SEQ, cols]).astype(BF16)
        used(3)
        hand_on(0, 2, 2, 3)
        next_w(mine_next, l + 1, 2, 3, 4, 5)

        @pl.when((l == 1) & (core == 0))
        def _():
            for j in (1, 0):
                for i in ALL:
                    push(i, j).start()
        save(U)
        save(E)
        return 0

    lax.fori_loop(0, LAYERS, layer, 0)
    y_here = pltpu.make_async_copy(do, y.at[rows], ysem.at[0])
    y_there = to_partner(do, y.at[rows], ysem.at[1], ysem.at[2])
    y_here.start()
    y_there.start()

    def free(chunk):
        @pl.when(chunk >= SENT_SLOTS)
        def _():
            cross(chunk).wait_send()

    def put(base, tile, value):
        q, half, unit = PLACE_OF[tile]
        index = jnp.where(core == half, own_slot(base + q), OWN_SLOTS + sent_slot(base + q))
        grads[index, unit] = value.reshape(CUBE + TILE)

    def ship(chunk):
        @pl.when(chunk >= SENT_SLOTS)
        def _():
            pl.semaphore_wait(credit.at[sent_slot(chunk)], 1)
        cross(chunk).start()

    def down_grad(base, halves):
        for half in halves:
            if half == 0:
                free(base)
                free(base + 1)
            w = dot_first(e[...], g[:, half * 256:half * 256 + 256]).reshape((64, QUAD, 8, 256))
            for j in range(2):
                for rg in range(QUAD):
                    put(base, (DOWN_W, rg, 2 * half + j), w[:, rg, :, j * LN:j * LN + LN])
            if half == 1:
                ship(base)

    def gelu_part(lo, hi):
        de = dot_last(g[...], vd[lo:hi, :])
        u[:, lo:hi] = (gelu_slope(u[:, lo:hi].astype(F32)) * de).astype(BF16)

    def wide_grad(base, array, a, b, parts):
        for part in parts:
            w = dot_first(a, b[:, part * D:part * D + D]).reshape((64, 8, D))
            for j in range(QUAD):
                put(base, (array, 0, QUAD * part + j), w[:, :, j * LN:j * LN + LN])

    seed_in.wait()
    down_grad(0, range(2))
    act(E, LAYERS - 2, True).start()
    y_here.wait()
    y_there.wait_send()

    def iteration(it, _):
        l = LAYERS - 1 - it
        more = it < LAYERS - 1
        base = 4 * it

        def loaded(acts_of, pieces=()):
            @pl.when(it > 0)
            def _():
                for i in acts_of:
                    act(i, l, True).wait()
                wait_w(*pieces)

        def after(acts_of, pieces=()):
            @pl.when(more)
            def _():
                for i in pieces:
                    fetch_w(i, l - 1, l <= 2)
                for i in acts_of:
                    act(i, l - 1, True).start()

        def piece(n):
            if n == 0:
                loaded((U,), DOWN_P)
                gelu_part(0, 3 * 256)
            elif n == 1:
                gelu_part(3 * 256, 3 * D)
            elif n == 2:
                gelu_part(3 * D, QUAD * D)
                after((), DOWN_P)
                loaded((M,))
                mf = m[...].astype(F32)
                g1[...] = (mf * inv_rms(mf)).astype(BF16)
                wide_grad(base, UP_W, g1[...], u, (0,))
            elif n == 3:
                free(base + 2)
                wide_grad(base, UP_W, g1[...], u, (1, 2, 3))
                ship(base + 1)
            elif n == 4:
                loaded((), UP_P)
                dc = dot_last(u[...], vu[...])
                g1[...] = (g[...].astype(F32) + rms_bwd(m[...].astype(F32), dc)).astype(BF16)
                after((U, M), UP_P)
            elif n == 5:
                loaded((O,), OUT_P)
                do[...] = dot_last(g1[...], vo[...]).astype(BF16)
                wide_grad(base, OUT_W, o[...], g1, (0,))
                ship(base + 2)
                after((O,), OUT_P)
            elif n in (6, 7):
                if n == 6:
                    loaded((PROB, QKV))
                attention_bwd(n - 6, BWD_SEQS, qkv, p, do)
                if n == 7:
                    after((PROB,))
            elif n == 8:
                loaded((H,))
                free(base + 3)
                hf = h[...].astype(F32)
                wide_grad(base, QKV_W, (hf * inv_rms(hf)).astype(BF16), qkv, range(3))
                ship(base + 3)
            elif n == 9:
                loaded((), QKV_P)
                da = dot_last(qkv[...], vq[...])
                g[...] = (g1[...].astype(F32) + rms_bwd(h[...].astype(F32), da)).astype(BF16)
                after((H, QKV), QKV_P)
            else:
                @pl.when(more)
                def _():
                    if n == 10:
                        act(E, l - 1, True).wait()
                    down_grad(base + QUAD, (n - 10,))

                if n == 11:
                    @pl.when(l > 1)
                    def _():
                        act(E, l - 2, True).start()

        for n in range(12):
            s = 12 * it + n - LEAD
            step = rings.step_of(n + 2 * PERIOD - LEAD)
            if n < LEAD:
                @pl.when(it > 0)
                def _():
                    rings.slot(s, step)
            else:
                rings.slot(s, step)
            piece(n)
        return 0

    lax.fori_loop(0, LAYERS, iteration, 0)
    rings.drain(SLOTS - LEAD)

    for q in range(SENT_SLOTS):
        cross(q).wait_send()
    last = to_partner(done.at[pl.ds(8 * core, 8)], out.at[core], fsem.at[0], fsem.at[1])
    last.start()
    kept = pltpu.make_async_copy(done.at[pl.ds(8 * (1 - core), 8)], out.at[core], gsem)
    kept.start()
    for j in range(2):
        for i in ALL:
            push(i, j).wait_send()

    @pl.when(core == 0)
    def _():
        for i in ALL:
            hand(i, 0).wait_send()
    y_there.wait_recv()
    kept.wait()
    last.wait_send()
    last.wait_recv()


def train_step(x, seed, weights):
    anywhere = pl.BlockSpec(memory_space=pl.ANY)
    dma = pltpu.SemaphoreType.DMA
    act = lambda cols, dt=BF16: pltpu.VMEM((ROWS, cols), dt)
    saved = lambda cols, dt=BF16: jax.ShapeDtypeStruct((LAYERS - 1, ROWS, cols), dt)
    outs = pl.pallas_call(
        step_kernel,
        name="step",
        out_shape=[jax.ShapeDtypeStruct((2 * ROWS, D), BF16)] + [jax.ShapeDtypeStruct((2,) + s, BF16) for s in W_SHAPES]
        + [saved(D), saved(3 * D), saved(2 * D, F32), saved(D), saved(D), saved(QUAD * D), saved(QUAD * D)]
        + [jax.ShapeDtypeStruct((2, 8, NU) + TILE, F32)],
        in_specs=[anywhere] * 6,
        out_specs=[anywhere] * 13,
        scratch_shapes=[
            pltpu.VMEM((OWN_SLOTS + SENT_SLOTS, NU) + CUBE + TILE, F32),
            pltpu.VMEM((SENT_SLOTS, NU) + CUBE + TILE, F32),
            pltpu.VMEM((CHUNKS, NU) + TILE, F32),
            act(D), act(3 * D), act(2 * D, F32), act(D), act(D), act(QUAD * D), act(QUAD * D), act(D), act(D), act(D),
        ] + [pltpu.VMEM(s, BF16) for s in W_SHAPES] + [
            dma((6,)), dma((7,)), dma, dma((6, 2)), dma((6, 2)), dma((2, 6)), dma((3,)), dma((QUAD,)), dma((QUAD,)), dma((2,)),
            pltpu.SemaphoreType.REGULAR((QUAD,)), pltpu.SemaphoreType.REGULAR((QUAD,)),
        ] + ring_scratch(),
        compiler_params=pltpu.CompilerParams(collective_id=1, has_side_effects=True, vmem_limit_bytes=67043328),
    )(x, seed, *weights)
    return outs[0], outs[-1]


ROW_SHAPES = ((2, 8, 3 * D), (2, 8, D), (2, 8, QUAD * D), (2, 32, D))


def finish_kernel(y_in, sums_in, y, gq, go, gu, gd, buf, sums, bq, bo, bu, bd, in_sem, out_sem, sum_sem, grad_sem):
    parts = buf.shape[0]
    here = pltpu.make_async_copy(sums_in, sums, sum_sem)
    here.start()
    into = [pltpu.make_async_copy(y_in.at[i], buf.at[i], in_sem.at[i]) for i in range(parts)]
    out = [pltpu.make_async_copy(buf.at[i], y.at[i], out_sem.at[i]) for i in range(parts)]
    for c in into:
        c.start()
    here.wait()
    rows = (bq, bo, bu, bd)
    for layer in range(2):
        for tile in TILES:
            array, rg, col = tile
            q, half, unit = PLACE_OF[tile]
            rows[array][layer, rg * 8:rg * 8 + 8, col * LN:col * LN + LN] = sums[half, QUAD * (1 - layer) + q, unit]
    out += [pltpu.make_async_copy(r, o, grad_sem.at[i]) for i, (r, o) in enumerate(zip(rows, (gq, go, gu, gd)))]
    for c, d in zip(into, out):
        c.wait()
        d.start()
    for d in out[parts:]:
        d.start()
    for d in out:
        d.wait()


def finish(y, sums, parts=6):
    anywhere = pl.BlockSpec(memory_space=pl.ANY)
    dma = pltpu.SemaphoreType.DMA
    shape = (parts, 2 * ROWS // parts, D)
    return pl.pallas_call(
        finish_kernel,
        name="finish",
        out_shape=[jax.ShapeDtypeStruct(shape, BF16)] + [jax.ShapeDtypeStruct(s, F32) for s in ROW_SHAPES],
        in_specs=[anywhere] * 2,
        out_specs=[anywhere] * 5,
        scratch_shapes=[pltpu.VMEM(shape, BF16), pltpu.VMEM(sums.shape, F32)] + [pltpu.VMEM(s, F32) for s in ROW_SHAPES]
        + [dma((parts,)), dma((parts,)), dma, dma((QUAD,))],
    )(y.reshape(shape), sums)


def solution(mesh):
    def step(x_in, seed_grad, w_qkv, w_out, w_up, w_down):
        shape = x_in.shape
        weights = (w_qkv, w_out, w_up, w_down)
        y, sums = train_step(x_in.reshape(2 * ROWS, D), seed_grad.reshape(2 * ROWS, D), weights)
        y, *grads = finish(y, sums)
        return y.reshape(shape), *grads

    act, weight, grad = P(None, "dp"), P("pp"), P("pp", "dp")
    return jax.shard_map(
        step,
        mesh=mesh,
        in_specs=(act, act, weight, weight, weight, weight),
        out_specs=(act, grad, grad, grad, grad),
        check_vma=False,
    )
```
